8 devices in a mesh: dp: 1 (over z), sp: 2 (over y), tp: 4 (over x, core).
Axes of the slice: x: 2, y: 2, z: 1, core: 2. Of those that a mesh axis runs over, the one named last changes fastest.
Arguments:
- x_in: bfloat16 [64, 128, 32, 256], P('dp', 'sp', None, 'tp')
- act_saved: bfloat16 [64, 128, 32, 256], P('dp', 'sp', None, 'tp')
- w_one: bfloat16 [3, 3, 256, 256], P(None, None, 'tp')
- w_two: bfloat16 [3, 3, 256, 256], P(None, None, 'tp')
- d_out: bfloat16 [64, 128, 32, 256], P('dp', 'sp', None, 'tp')
Outputs:
- output 1: bfloat16 [64, 128, 32, 256], P('dp', 'sp', None, 'tp')
- output 2: float32 [3, 3, 256, 256], P('dp', None, 'tp')
- output 3: float32 [3, 3, 256, 256], P('dp', None, 'tp')
- output 4: float32 [256], P(('dp', 'tp'))
All inputs are finite; a program needn't handle non-finite values.
Results may differ from the reference program's by a relative error of at most 0.001.
Values are sent between devices in bfloat16 or wider.
A program may use at most 1 GiB of HBM per device.

```python
import jax
import jax.numpy as jnp
from jax import lax

BATCH_SIZE = 64
HEIGHT = 128
IMG_WIDTH = 32
CHANNELS = 256


def setup_inputs(seed: int = 0, part: int = 0) -> dict:
    part_key = jax.random.fold_in(jax.random.key(seed), part)
    key_list = jax.random.split(part_key, 3)
    shared_list = jax.random.split(jax.random.key(seed + 1), 2)
    arr_shape = (BATCH_SIZE, HEIGHT, IMG_WIDTH, CHANNELS)
    kern_shape = (3, 3, CHANNELS, CHANNELS)
    kern_scale = (9 * CHANNELS) ** -0.5
    x_in = jax.random.normal(key_list[0], arr_shape, jnp.float32).astype(jnp.bfloat16)
    act_saved = jnp.maximum(jax.random.normal(key_list[1], arr_shape, jnp.float32), 0.0).astype(jnp.bfloat16)
    d_out = jax.random.normal(key_list[2], arr_shape, jnp.float32).astype(jnp.bfloat16)
    w_one = (jax.random.normal(shared_list[0], kern_shape, jnp.float32) * kern_scale).astype(jnp.bfloat16)
    w_two = (jax.random.normal(shared_list[1], kern_shape, jnp.float32) * kern_scale).astype(jnp.bfloat16)
    return {"x_in": x_in, "act_saved": act_saved, "w_one": w_one, "w_two": w_two, "d_out": d_out}


def conv_forward(image, kernel):
    return lax.conv_general_dilated(image, kernel, (1, 1), "SAME", dimension_numbers=("NHWC", "HWIO", "NHWC"))


def reference(x_in, act_saved, w_one, w_two, d_out):
    cot_out = d_out.astype(jnp.float32)
    pull_two = jax.vjp(conv_forward, act_saved.astype(jnp.float32), w_two.astype(jnp.float32))[1]
    d_act, grad_two = pull_two(cot_out)
    masked = jnp.where(act_saved > 0, d_act, 0.0)
    grad_bias = jnp.sum(masked, axis=(0, 1, 2))
    d_pre = masked.astype(jnp.bfloat16).astype(jnp.float32)
    pull_one = jax.vjp(conv_forward, x_in.astype(jnp.float32), w_one.astype(jnp.float32))[1]
    d_conv, grad_one = pull_one(d_pre)
    d_x = (cot_out + d_conv).astype(jnp.bfloat16)
    return d_x, grad_one, grad_two, grad_bias
```

```python
import jax
import jax.numpy as jnp
from jax import lax
from jax.experimental import pallas as pl
from jax.experimental.pallas import tpu as pltpu
from jax.sharding import PartitionSpec as P

MESH = pl.DeviceIdType.MESH
F32, BF16 = jnp.float32, jnp.bfloat16
TAPS = 9
CONV_ROWS = 16
GRAD_ROWS = 32


def body(num, rows, width, x_hbm, a_hbm, y_hbm, w1_ref, w2_ref, dx_hbm, acc1, acc2, db_ref,
         nat_own, nat_rem, g_own, g_oth, z_own, z_oth, shifted, out_own, out_rem,
         load_sem, push_send, push_recv, g_send, g_recv, z_send, z_recv, out_sem, out_send, out_recv, free_sem):
    dp, sp, tp = lax.axis_index("dp"), lax.axis_index("sp"), lax.axis_index("tp")
    core = tp % 2
    partner = (dp, sp, tp + 1 - 2 * core)
    across = (dp, sp, (tp + 2) % 4)
    beside = (dp, 1 - sp, tp)
    diagonal = (dp, 1 - sp, (tp + 2) % 4)
    peers = (partner, across, beside, diagonal)
    half = 64
    lanes = 2 * half
    edge_row = (rows + 1) * sp
    halo_row = (rows + 1) * (1 - sp)
    halo_src = rows - (rows - 1) * sp
    m_conv = CONV_ROWS * width
    m_grad = GRAD_ROWS * width

    barrier = pltpu.get_barrier_semaphore()
    for peer in peers:
        pl.semaphore_signal(barrier, inc=1, device_id=peer, device_id_type=MESH)
    pl.semaphore_wait(barrier, 4)

    def remote(src, dst, send, recv, peer):
        return pltpu.make_async_remote_copy(src_ref=src, dst_ref=dst, send_sem=send, recv_sem=recv, device_id=peer, device_id_type=MESH)

    sources = (y_hbm, a_hbm, x_hbm)

    def loads(kind, img):
        slot = img % 2
        local = pltpu.make_async_copy(sources[kind].at[core * num + img], nat_own.at[kind, slot], load_sem.at[kind, slot])
        push = remote(sources[kind].at[(1 - core) * num + img], nat_rem.at[kind, slot], push_send.at[kind, slot], push_recv.at[kind, slot], partner)
        return local, push

    def start_loads(kind, img):
        for copy in loads(kind, img):
            copy.start()

    def wait_loads(kind, img):
        for copy in loads(kind, img):
            copy.wait()

    def exchange(own, own_slot, oth, oth_slot, send, recv, sem_slot):
        return (
            remote(own.at[own_slot, pl.ds(1, rows)], oth.at[oth_slot, pl.ds(1, rows)], send.at[0, sem_slot], recv.at[0, sem_slot], across),
            remote(own.at[own_slot, halo_src], own.at[own_slot, edge_row], send.at[1, sem_slot], recv.at[1, sem_slot], beside),
            remote(own.at[own_slot, halo_src], oth.at[oth_slot, edge_row], send.at[2, sem_slot], recv.at[2, sem_slot], diagonal),
        )

    def g_exchange(img):
        return exchange(g_own, img % 3, g_oth, img % 2, g_send, g_recv, img % 2)

    def z_exchange(img):
        return exchange(z_own, img % 2, z_oth, img % 2, z_send, z_recv, img % 2)

    def out_copies(img):
        slot = img % 2
        local = pltpu.make_async_copy(out_own.at[slot], dx_hbm.at[core * num + img], out_sem.at[slot])
        push = remote(out_rem.at[slot], dx_hbm.at[core * num + img], out_send.at[slot], out_recv.at[img % 4], partner)
        return local, push

    def wait_out(img):
        for copy in out_copies(img):
            copy.wait()

    def dense(kind, slot, r0, count):
        mine = nat_own[kind, slot, pl.ds(r0, count)]
        theirs = nat_rem[kind, slot, pl.ds(r0, count)]
        return jnp.concatenate([mine, theirs], axis=-1)

    zero_row = jnp.zeros((width, lanes), BF16)
    for slot in range(3):
        g_own[slot, edge_row] = zero_row
    for slot in range(2):
        g_oth[slot, edge_row] = zero_row
        z_own[slot, edge_row] = zero_row
        z_oth[slot, edge_row] = zero_row
    for side in range(3):
        for row in (0, 1, rows + 2, rows + 3):
            shifted[side, row] = zero_row
    acc1[...] = jnp.zeros_like(acc1)
    acc2[...] = jnp.zeros_like(acc2)
    db_ref[...] = jnp.zeros_like(db_ref)

    col = lax.broadcasted_iota(jnp.int32, (m_conv, lanes), 0) % width
    at_first = col == 0
    at_last = col == width - 1

    def from_right(v):
        return jnp.where(at_last, 0.0, pltpu.roll(v, m_conv - 1, 0))

    def from_left(v):
        return jnp.where(at_first, 0.0, pltpu.roll(v, 1, 0))

    def prepare(kind, img):
        @pl.loop(0, rows // CONV_ROWS)
        def _(k):
            r0 = k * CONV_ROWS
            v = dense(kind, img % 2, r0, CONV_ROWS)
            flat = v.reshape(m_conv, lanes).astype(F32)
            shifted[1, pl.ds(r0 + 2, CONV_ROWS)] = v
            shifted[0, pl.ds(r0 + 2, CONV_ROWS)] = from_left(flat).astype(BF16).reshape(v.shape)
            shifted[2, pl.ds(r0 + 2, CONV_ROWS)] = from_right(flat).astype(BF16).reshape(v.shape)

    def both(own, oth, r, count):
        shape = (count * width, lanes)
        return [own[pl.ds(r, count)].reshape(shape), oth[pl.ds(r, count)].reshape(shape)]

    def conv(own, oth, r0, w_ref):
        lhs = jnp.concatenate(sum((both(own, oth, r0 + 2 - kh, CONV_ROWS) for kh in range(3)), []), axis=-1)
        out = jnp.dot(lhs, w_ref[...], preferred_element_type=F32)
        return out[:, lanes:2 * lanes] + from_right(out[:, :lanes]) + from_left(out[:, 2 * lanes:])

    def kgrad(own, oth, acc):
        def piece(r, count):
            lhs = jnp.concatenate(both(own, oth, r, count), axis=-1)
            taps = [shifted[kw, pl.ds(r + kh, count)].reshape(count * width, lanes) for kh in range(3) for kw in range(3)]
            rhs = jnp.concatenate(taps, axis=-1)
            acc[...] += lax.dot_general(lhs, rhs, (((0,), (0,)), ((), ())), preferred_element_type=F32)

        @pl.loop(0, rows // GRAD_ROWS)
        def _(k):
            piece(1 + k * GRAD_ROWS, GRAD_ROWS)

        piece(halo_row, 1)

    def first(img):
        own, oth = g_own.at[img % 3], g_oth.at[img % 2]
        out = z_own.at[img % 2]

        @pl.loop(0, rows // CONV_ROWS)
        def _(k):
            r0 = k * CONV_ROWS
            d_act = conv(own, oth, r0, w2_ref)
            live = shifted[1, pl.ds(r0 + 2, CONV_ROWS)].reshape(m_conv, lanes).astype(F32) > 0
            masked = jnp.where(live, d_act, 0.0)
            db_ref[...] += jnp.sum(masked.reshape(m_conv // 8, 8, lanes), axis=0)
            out[pl.ds(1 + r0, CONV_ROWS)] = masked.astype(BF16).reshape(CONV_ROWS, width, lanes)

    def second(img):
        own, oth = z_own.at[img % 2], z_oth.at[img % 2]
        skip = g_own.at[img % 3]
        slot = img % 2

        @pl.loop(0, rows // CONV_ROWS)
        def _(k):
            r0 = k * CONV_ROWS
            d_x = conv(own, oth, r0, w1_ref)
            d_x = d_x + skip[pl.ds(1 + r0, CONV_ROWS)].reshape(m_conv, lanes).astype(F32)
            d_x = d_x.astype(BF16).reshape(CONV_ROWS, width, lanes)
            out_own[slot, pl.ds(r0, CONV_ROWS)] = d_x[..., :half]
            out_rem[slot, pl.ds(r0, CONV_ROWS)] = d_x[..., half:]

    start_loads(0, 0)
    steps = num + 2

    @pl.loop(0, steps)
    def _(step):
        @pl.when(step >= 1)
        def _():
            for rel in range(4):
                pl.semaphore_wait(free_sem.at[rel], 1)

        @pl.when(step + 1 < num)
        def _():
            start_loads(0, step + 1)

        @pl.when(step < num)
        def _():
            start_loads(1, step)
            wait_loads(0, step)
            dst = g_own.at[step % 3]

            @pl.loop(0, rows // CONV_ROWS)
            def _(k):
                dst[pl.ds(1 + k * CONV_ROWS, CONV_ROWS)] = dense(0, step % 2, k * CONV_ROWS, CONV_ROWS)

            for copy in g_exchange(step):
                copy.start()

        @pl.when((step >= 1) & (step <= num))
        def _():
            img = step - 1
            start_loads(2, img)
            wait_loads(1, img)
            prepare(1, img)
            for copy in g_exchange(img):
                copy.wait()
            first(img)
            for copy in z_exchange(img):
                copy.start()
            kgrad(g_own.at[img % 3], g_oth.at[img % 2], acc2)

        @pl.when(step >= 2)
        def _():
            img = step - 2
            wait_loads(2, img)
            prepare(2, img)

            @pl.when(img >= 2)
            def _():
                wait_out(img - 2)

            for copy in z_exchange(img):
                copy.wait()
            second(img)
            for copy in out_copies(img):
                copy.start()
            kgrad(z_own.at[img % 2], z_oth.at[img % 2], acc1)

        @pl.when(step + 1 < steps)
        def _():
            for rel, peer in enumerate(peers):
                pl.semaphore_signal(free_sem.at[rel], inc=1, device_id=peer, device_id_type=MESH)

    wait_out(num - 2)
    wait_out(num - 1)


def solution(mesh):
    def local_step(x_in, act_saved, w_one, w_two, d_out):
        images, rows, width, half = x_in.shape
        num = images // 2
        lanes = 2 * half
        tp = lax.axis_index("tp")
        swap_cores = [(t, t ^ 1) for t in range(4)]
        swap_rows = [(0, 1), (1, 0)]

        kernels = jnp.stack([w_one, w_two])
        kernels = jnp.concatenate([kernels, lax.ppermute(kernels, "tp", swap_cores)], axis=3)

        def reorder(arr, axis):
            pieces = [lax.dynamic_slice_in_dim(arr, jnp.bitwise_xor(tp, b) * half, half, axis) for b in range(4)]
            return jnp.concatenate(pieces, axis=axis)

        kernels = reorder(kernels, 4).transpose(0, 1, 4, 2, 3).reshape(2, 3 * 4 * half, 3 * lanes)
        pad = (rows + 2, width, lanes)
        dma = pltpu.SemaphoreType.DMA
        hbm = pl.BlockSpec(memory_space=pltpu.HBM)
        vmem = pl.BlockSpec(memory_space=pltpu.VMEM)
        d_x, acc1, acc2, bias = pl.pallas_call(
            lambda *refs: body(num, rows, width, *refs),
            out_shape=(
                jax.ShapeDtypeStruct(x_in.shape, BF16),
                jax.ShapeDtypeStruct((4 * half, TAPS * lanes), F32),
                jax.ShapeDtypeStruct((4 * half, TAPS * lanes), F32),
                jax.ShapeDtypeStruct((8, lanes), F32),
            ),
            in_specs=[hbm, hbm, hbm, vmem, vmem],
            out_specs=[hbm, vmem, vmem, vmem],
            scratch_shapes=[
                pltpu.VMEM((3, 2, rows, width, half), BF16),
                pltpu.VMEM((3, 2, rows, width, half), BF16),
                pltpu.VMEM((3,) + pad, BF16),
                pltpu.VMEM((2,) + pad, BF16),
                pltpu.VMEM((2,) + pad, BF16),
                pltpu.VMEM((2,) + pad, BF16),
                pltpu.VMEM((3, rows + 4, width, lanes), BF16),
                pltpu.VMEM((2, rows, width, half), BF16),
                pltpu.VMEM((2, rows, width, half), BF16),
                dma((3, 2)), dma((3, 2)), dma((3, 2)),
                dma((3, 2)), dma((3, 2)), dma((3, 2)), dma((3, 2)),
                dma((2,)), dma((2,)), dma((4,)),
                pltpu.SemaphoreType.REGULAR((4,)),
            ],
            compiler_params=pltpu.CompilerParams(collective_id=0, has_side_effects=True, vmem_limit_bytes=60 * 1024 * 1024),
        )(x_in, act_saved, d_out, kernels[0], kernels[1])

        sums = jnp.stack([acc1, acc2]).reshape(2, 4 * half, TAPS, lanes)
        sums = reorder(sums, 1)
        bias = jnp.sum(bias, axis=0)
        mine, theirs = sums[..., :half], sums[..., half:]
        mine = mine + lax.ppermute(theirs, "tp", swap_cores)
        bias = bias[:half] + lax.ppermute(bias[half:], "tp", swap_cores)
        mine = mine.transpose(0, 2, 3, 1)
        mine = mine + lax.ppermute(mine, "sp", swap_rows)
        bias = bias + lax.ppermute(bias, "sp", swap_rows)
        grads = mine.reshape(2, 3, 3, half, 4 * half)
        return d_x, grads[0], grads[1], bias

    act_spec = P("dp", "sp", None, "tp")
    kern_spec = P(None, None, "tp", None)
    grad_spec = P("dp", None, "tp", None)
    return jax.shard_map(local_step, mesh=mesh, in_specs=(act_spec, act_spec, kern_spec, kern_spec, act_spec), out_specs=(act_spec, grad_spec, grad_spec, P(("dp", "tp"))), check_vma=False)
```

```python
import jax
import jax.numpy as jnp
from jax import lax
from jax.experimental import pallas as pl
from jax.experimental.pallas import tpu as pltpu
from jax.sharding import PartitionSpec as P

MESH = pl.DeviceIdType.MESH
F32, BF16 = jnp.float32, jnp.bfloat16
TAPS = 9
CONV_ROWS = 16
GRAD_ROWS = 32


def body(num, rows, width, x_hbm, a_hbm, y_hbm, w1_ref, w2_ref, dx_hbm, acc1, acc2, db_ref,
         nat_own, nat_rem, g_own, g_oth, z_own, z_oth, shifted, out_own, out_rem,
         load_sem, push_send, push_recv, g_send, g_recv, z_send, z_recv, out_sem, out_send, out_recv, free_sem):
    dp, sp, tp = lax.axis_index("dp"), lax.axis_index("sp"), lax.axis_index("tp")
    core = tp % 2
    partner = (dp, sp, tp + 1 - 2 * core)
    across = (dp, sp, (tp + 2) % 4)
    beside = (dp, 1 - sp, tp)
    peers = (partner, across, beside)
    half = 64
    lanes = 2 * half
    edge_row = (rows + 1) * sp
    halo_row = (rows + 1) * (1 - sp)
    halo_src = rows - (rows - 1) * sp
    m_conv = CONV_ROWS * width
    m_grad = GRAD_ROWS * width

    barrier = pltpu.get_barrier_semaphore()
    for peer in peers:
        pl.semaphore_signal(barrier, inc=1, device_id=peer, device_id_type=MESH)
    pl.semaphore_wait(barrier, 3)

    def remote(src, dst, send, recv, peer):
        return pltpu.make_async_remote_copy(src_ref=src, dst_ref=dst, send_sem=send, recv_sem=recv, device_id=peer, device_id_type=MESH)

    sources = (y_hbm, a_hbm, x_hbm)

    def loads(kind, img):
        slot = img % 2
        local = pltpu.make_async_copy(sources[kind].at[core * num + img], nat_own.at[kind, slot], load_sem.at[kind, slot])
        push = remote(sources[kind].at[(1 - core) * num + img], nat_rem.at[kind, slot], push_send.at[kind, slot], push_recv.at[kind, slot], partner)
        return local, push

    def start_loads(kind, img):
        for copy in loads(kind, img):
            copy.start()

    def wait_loads(kind, img):
        for copy in loads(kind, img):
            copy.wait()

    def exchange(own, own_slot, oth, oth_slot, send, recv, sem_slot):
        return (
            remote(own.at[own_slot, pl.ds(1, rows)], oth.at[oth_slot, pl.ds(1, rows)], send.at[0, sem_slot], recv.at[0, sem_slot], across),
            remote(own.at[own_slot, halo_src], own.at[own_slot, edge_row], send.at[1, sem_slot], recv.at[1, sem_slot], beside),
            remote(oth.at[oth_slot, halo_src], oth.at[oth_slot, edge_row], send.at[2, sem_slot], recv.at[2, sem_slot], beside),
        )

    def g_exchange(img):
        return exchange(g_own, img % 3, g_oth, img % 2, g_send, g_recv, img % 2)

    def z_exchange(img):
        return exchange(z_own, img % 2, z_oth, img % 2, z_send, z_recv, img % 2)

    def swap_out(img):
        slot = img % 2
        return remote(out_own.at[slot], out_rem.at[slot], out_send.at[slot], out_recv.at[slot], partner)

    def store_out(img):
        return pltpu.make_async_copy(out_own.at[img % 2], dx_hbm.at[img], out_sem.at[img % 2])

    def finish_out(img):
        slot = img % 2
        swap_out(img).wait()

        @pl.loop(0, rows // CONV_ROWS)
        def _(k):
            block = pl.ds(k * CONV_ROWS, CONV_ROWS)
            lane = lax.broadcasted_iota(jnp.int32, (CONV_ROWS, width, lanes), 2)
            out_own[slot, block] = jnp.where(lane < half, out_own[slot, block], out_rem[slot, block])

        store_out(img).start()

    def dense(kind, slot, r0, count):
        mine = nat_own[kind, slot, pl.ds(r0, count)]
        theirs = nat_rem[kind, slot, pl.ds(r0, count)]
        return jnp.concatenate([mine, theirs], axis=-1)

    zero_row = jnp.zeros((width, lanes), BF16)
    for slot in range(3):
        g_own[slot, edge_row] = zero_row
    for slot in range(2):
        g_oth[slot, edge_row] = zero_row
        z_own[slot, edge_row] = zero_row
        z_oth[slot, edge_row] = zero_row
    for side in range(3):
        for row in (0, 1, rows + 2, rows + 3):
            shifted[side, row] = zero_row
    acc1[...] = jnp.zeros_like(acc1)
    acc2[...] = jnp.zeros_like(acc2)
    db_ref[...] = jnp.zeros_like(db_ref)

    col = lax.broadcasted_iota(jnp.int32, (m_conv, lanes), 0) % width
    at_first = col == 0
    at_last = col == width - 1

    def from_right(v):
        return jnp.where(at_last, 0.0, pltpu.roll(v, m_conv - 1, 0))

    def from_left(v):
        return jnp.where(at_first, 0.0, pltpu.roll(v, 1, 0))

    def prepare(kind, img):
        @pl.loop(0, rows // CONV_ROWS)
        def _(k):
            r0 = k * CONV_ROWS
            v = dense(kind, img % 2, r0, CONV_ROWS)
            flat = v.reshape(m_conv, lanes).astype(F32)
            shifted[1, pl.ds(r0 + 2, CONV_ROWS)] = v
            shifted[0, pl.ds(r0 + 2, CONV_ROWS)] = from_left(flat).astype(BF16).reshape(v.shape)
            shifted[2, pl.ds(r0 + 2, CONV_ROWS)] = from_right(flat).astype(BF16).reshape(v.shape)

    def both(own, oth, r, count):
        shape = (count * width, lanes)
        return [own[pl.ds(r, count)].reshape(shape), oth[pl.ds(r, count)].reshape(shape)]

    def conv(own, oth, r0, w_ref):
        lhs = jnp.concatenate(sum((both(own, oth, r0 + 2 - kh, CONV_ROWS) for kh in range(3)), []), axis=-1)
        out = jnp.dot(lhs, w_ref[...], preferred_element_type=F32)
        return out[:, lanes:2 * lanes] + from_right(out[:, :lanes]) + from_left(out[:, 2 * lanes:])

    def kgrad(own, oth, acc):
        def piece(r, count):
            lhs = jnp.concatenate(both(own, oth, r, count), axis=-1)
            taps = [shifted[kw, pl.ds(r + kh, count)].reshape(count * width, lanes) for kh in range(3) for kw in range(3)]
            rhs = jnp.concatenate(taps, axis=-1)
            acc[...] += lax.dot_general(lhs, rhs, (((0,), (0,)), ((), ())), preferred_element_type=F32)

        @pl.loop(0, rows // GRAD_ROWS)
        def _(k):
            piece(1 + k * GRAD_ROWS, GRAD_ROWS)

        piece(halo_row, 1)

    last_block = rows // CONV_ROWS - 1

    def blocks(halo, step):
        @pl.loop(0, last_block + 1)
        def _(k):
            @pl.when(k == last_block)
            def _():
                halo.wait()

            step((k + (last_block - 2 * k) * sp) * CONV_ROWS)

    def first(img, halo):
        own, oth = g_own.at[img % 3], g_oth.at[img % 2]
        out = z_own.at[img % 2]

        def step(r0):
            d_act = conv(own, oth, r0, w2_ref)
            live = shifted[1, pl.ds(r0 + 2, CONV_ROWS)].reshape(m_conv, lanes).astype(F32) > 0
            masked = jnp.where(live, d_act, 0.0)
            db_ref[...] += jnp.sum(masked.reshape(m_conv // 8, 8, lanes), axis=0)
            out[pl.ds(1 + r0, CONV_ROWS)] = masked.astype(BF16).reshape(CONV_ROWS, width, lanes)

        blocks(halo, step)

    def second(img, halo):
        own, oth = z_own.at[img % 2], z_oth.at[img % 2]
        skip = g_own.at[img % 3]
        slot = img % 2

        def step(r0):
            d_x = conv(own, oth, r0, w1_ref)
            d_x = d_x + skip[pl.ds(1 + r0, CONV_ROWS)].reshape(m_conv, lanes).astype(F32)
            out_own[slot, pl.ds(r0, CONV_ROWS)] = d_x.astype(BF16).reshape(CONV_ROWS, width, lanes)

        blocks(halo, step)

    def arrive(copies):
        main, side, forward = copies
        main.wait()
        forward.start()
        side.wait()
        return forward

    start_loads(0, 0)
    steps = num + 2

    @pl.loop(0, steps)
    def _(step):
        @pl.when(step >= 1)
        def _():
            for rel in range(3):
                pl.semaphore_wait(free_sem.at[rel], 1)

        @pl.when(step + 1 < num)
        def _():
            start_loads(0, step + 1)

        @pl.when(step < num)
        def _():
            start_loads(1, step)
            wait_loads(0, step)
            dst = g_own.at[step % 3]

            @pl.loop(0, rows // CONV_ROWS)
            def _(k):
                dst[pl.ds(1 + k * CONV_ROWS, CONV_ROWS)] = dense(0, step % 2, k * CONV_ROWS, CONV_ROWS)

            for copy in g_exchange(step)[:2]:
                copy.start()

        @pl.when((step >= 1) & (step <= num))
        def _():
            img = step - 1
            start_loads(2, img)
            wait_loads(1, img)
            prepare(1, img)
            first(img, arrive(g_exchange(img)))
            for copy in z_exchange(img)[:2]:
                copy.start()
            kgrad(g_own.at[img % 3], g_oth.at[img % 2], acc2)

        @pl.when(step >= 2)
        def _():
            img = step - 2
            wait_loads(2, img)
            prepare(2, img)

            @pl.when(img >= 1)
            def _():
                finish_out(img - 1)

            @pl.when(img >= 2)
            def _():
                store_out(img - 2).wait()

            second(img, arrive(z_exchange(img)))
            swap_out(img).start()
            kgrad(z_own.at[img % 2], z_oth.at[img % 2], acc1)

        @pl.when(step + 1 < steps)
        def _():
            for rel, peer in enumerate(peers):
                pl.semaphore_signal(free_sem.at[rel], inc=1, device_id=peer, device_id_type=MESH)

    finish_out(num - 1)
    store_out(num - 2).wait()
    store_out(num - 1).wait()


def unpack(packed, out):
    core = lax.axis_index("tp") % 2
    half = out.shape[-1]
    out[core] = packed[..., :half]
    out[1 - core] = packed[..., half:]


def solution(mesh):
    def local_step(x_in, act_saved, w_one, w_two, d_out):
        images, rows, width, half = x_in.shape
        num = images // 2
        lanes = 2 * half
        tp = lax.axis_index("tp")
        swap_cores = [(t, t ^ 1) for t in range(4)]
        swap_rows = [(0, 1), (1, 0)]

        kernels = jnp.stack([w_one, w_two])
        kernels = jnp.concatenate([kernels, lax.ppermute(kernels, "tp", swap_cores)], axis=3)

        def reorder(arr, axis):
            pieces = [lax.dynamic_slice_in_dim(arr, jnp.bitwise_xor(tp, b) * half, half, axis) for b in range(4)]
            return jnp.concatenate(pieces, axis=axis)

        kernels = reorder(kernels, 4).transpose(0, 1, 4, 2, 3).reshape(2, 3 * 4 * half, 3 * lanes)
        pad = (rows + 2, width, lanes)
        dma = pltpu.SemaphoreType.DMA
        hbm = pl.BlockSpec(memory_space=pltpu.HBM)
        vmem = pl.BlockSpec(memory_space=pltpu.VMEM)
        packed, acc1, acc2, bias = pl.pallas_call(
            lambda *refs: body(num, rows, width, *refs),
            out_shape=(
                jax.ShapeDtypeStruct((num, rows, width, lanes), BF16),
                jax.ShapeDtypeStruct((4 * half, TAPS * lanes), F32),
                jax.ShapeDtypeStruct((4 * half, TAPS * lanes), F32),
                jax.ShapeDtypeStruct((8, lanes), F32),
            ),
            in_specs=[hbm, hbm, hbm, vmem, vmem],
            out_specs=[hbm, vmem, vmem, vmem],
            scratch_shapes=[
                pltpu.VMEM((3, 2, rows, width, half), BF16),
                pltpu.VMEM((3, 2, rows, width, half), BF16),
                pltpu.VMEM((3,) + pad, BF16),
                pltpu.VMEM((2,) + pad, BF16),
                pltpu.VMEM((2,) + pad, BF16),
                pltpu.VMEM((2,) + pad, BF16),
                pltpu.VMEM((3, rows + 4, width, lanes), BF16),
                pltpu.VMEM((2, rows, width, lanes), BF16),
                pltpu.VMEM((2, rows, width, lanes), BF16),
                dma((3, 2)), dma((3, 2)), dma((3, 2)),
                dma((3, 2)), dma((3, 2)), dma((3, 2)), dma((3, 2)),
                dma((2,)), dma((2,)), dma((2,)),
                pltpu.SemaphoreType.REGULAR((3,)),
            ],
            compiler_params=pltpu.CompilerParams(collective_id=0, has_side_effects=True, vmem_limit_bytes=60 * 1024 * 1024),
        )(x_in, act_saved, d_out, kernels[0], kernels[1])

        group = 2
        d_x = pl.pallas_call(
            unpack,
            grid=(num // group,),
            out_shape=jax.ShapeDtypeStruct((2, num, rows, width, half), BF16),
            in_specs=[pl.BlockSpec((group, rows, width, lanes), lambda i: (i, 0, 0, 0))],
            out_specs=pl.BlockSpec((2, group, rows, width, half), lambda i: (0, i, 0, 0, 0)),
            cost_estimate=pl.CostEstimate(flops=10**10, bytes_accessed=5 * 10**7, transcendentals=0),
        )(packed).reshape(x_in.shape)

        sums = jnp.stack([acc1, acc2]).reshape(2, 4 * half, TAPS, lanes)
        sums = reorder(sums, 1)
        bias = jnp.sum(bias, axis=0)
        mine, theirs = sums[..., :half], sums[..., half:]
        mine = mine + lax.ppermute(theirs, "tp", swap_cores)
        bias = bias[:half] + lax.ppermute(bias[half:], "tp", swap_cores)
        mine = mine.transpose(0, 2, 3, 1)
        mine = mine + lax.ppermute(mine, "sp", swap_rows)
        bias = bias + lax.ppermute(bias, "sp", swap_rows)
        grads = mine.reshape(2, 3, 3, half, 4 * half)
        return d_x, grads[0], grads[1], bias

    act_spec = P("dp", "sp", None, "tp")
    kern_spec = P(None, None, "tp", None)
    grad_spec = P("dp", None, "tp", None)
    return jax.shard_map(local_step, mesh=mesh, in_specs=(act_spec, act_spec, kern_spec, kern_spec, act_spec), out_specs=(act_spec, grad_spec, grad_spec, P(("dp", "tp"))), check_vma=False)
```

```python
import jax
import jax.numpy as jnp
from jax import lax
from jax.experimental import pallas as pl
from jax.experimental.pallas import tpu as pltpu
from jax.sharding import PartitionSpec as P

MESH = pl.DeviceIdType.MESH
F32, BF16 = jnp.float32, jnp.bfloat16
TAPS = 9
CONV_ROWS = 16
GRAD_ROWS = 32


def body(num, rows, width, x_hbm, a_hbm, y_hbm, w1_hbm, w2_hbm, dx_hbm, dw1_ref, dw2_ref,
         acc1, acc2, db_ref, raw_own, raw_rem, weights, part_own, part_send, part_recv, row_recv, nat_own, nat_rem, g_own, g_oth, z_own, z_oth, shifted, out_own, out_rem,
         load_sem, push_send, push_recv, g_send, g_recv, z_send, z_recv, out_sem, out_send, out_recv, raw_sem, raw_send, raw_recv, part_sems, free_sem):
    dp, sp, tp = lax.axis_index("dp"), lax.axis_index("sp"), lax.axis_index("tp")
    core, chip = tp % 2, tp // 2
    partner = (dp, sp, tp + 1 - 2 * core)
    across = (dp, sp, (tp + 2) % 4)
    beside = (dp, 1 - sp, tp)
    peers = (partner, across, beside)
    half = 64
    lanes = 2 * half
    edge_row = (rows + 1) * sp
    halo_row = (rows + 1) * (1 - sp)
    halo_src = rows - (rows - 1) * sp
    m_conv = CONV_ROWS * width
    m_grad = GRAD_ROWS * width

    barrier = pltpu.get_barrier_semaphore()
    for peer in peers:
        pl.semaphore_signal(barrier, inc=1, device_id=peer, device_id_type=MESH)
    pl.semaphore_wait(barrier, 3)

    def remote(src, dst, send, recv, peer):
        return pltpu.make_async_remote_copy(src_ref=src, dst_ref=dst, send_sem=send, recv_sem=recv, device_id=peer, device_id_type=MESH)

    sources = (y_hbm, a_hbm, x_hbm)

    def loads(kind, img):
        slot = img % 2
        local = pltpu.make_async_copy(sources[kind].at[core * num + img], nat_own.at[kind, slot], load_sem.at[kind, slot])
        push = remote(sources[kind].at[(1 - core) * num + img], nat_rem.at[kind, slot], push_send.at[kind, slot], push_recv.at[kind, slot], partner)
        return local, push

    def start_loads(kind, img):
        for copy in loads(kind, img):
            copy.start()

    def wait_loads(kind, img):
        for copy in loads(kind, img):
            copy.wait()

    def exchange(own, own_slot, oth, oth_slot, send, recv, sem_slot):
        return (
            remote(own.at[own_slot, pl.ds(1, rows)], oth.at[oth_slot, pl.ds(1, rows)], send.at[0, sem_slot], recv.at[0, sem_slot], across),
            remote(own.at[own_slot, halo_src], own.at[own_slot, edge_row], send.at[1, sem_slot], recv.at[1, sem_slot], beside),
            remote(oth.at[oth_slot, halo_src], oth.at[oth_slot, edge_row], send.at[2, sem_slot], recv.at[2, sem_slot], beside),
        )

    def g_exchange(img):
        return exchange(g_own, img % 3, g_oth, img % 2, g_send, g_recv, img % 2)

    def z_exchange(img):
        return exchange(z_own, img % 2, z_oth, img % 2, z_send, z_recv, img % 2)

    def swap_out(img):
        slot = img % 2
        return remote(out_own.at[slot], out_rem.at[slot], out_send.at[slot], out_recv.at[slot], partner)

    def store_out(img):
        return pltpu.make_async_copy(out_own.at[img % 2], dx_hbm.at[img], out_sem.at[img % 2])

    def finish_out(img):
        slot = img % 2
        swap_out(img).wait()

        @pl.loop(0, rows // CONV_ROWS)
        def _(k):
            block = pl.ds(k * CONV_ROWS, CONV_ROWS)
            lane = lax.broadcasted_iota(jnp.int32, (CONV_ROWS, width, lanes), 2)
            out_own[slot, block] = jnp.where(lane < half, out_own[slot, block], out_rem[slot, block])

        store_out(img).start()

    def dense(kind, slot, r0, count):
        mine = nat_own[kind, slot, pl.ds(r0, count)]
        theirs = nat_rem[kind, slot, pl.ds(r0, count)]
        return jnp.concatenate([mine, theirs], axis=-1)

    col = lax.broadcasted_iota(jnp.int32, (m_conv, lanes), 0) % width
    at_first = col == 0
    at_last = col == width - 1

    def from_right(v):
        return jnp.where(at_last, 0.0, pltpu.roll(v, m_conv - 1, 0))

    def from_left(v):
        return jnp.where(at_first, 0.0, pltpu.roll(v, 1, 0))

    def prepare(kind, img):
        @pl.loop(0, rows // CONV_ROWS)
        def _(k):
            r0 = k * CONV_ROWS
            v = dense(kind, img % 2, r0, CONV_ROWS)
            flat = v.reshape(m_conv, lanes).astype(F32)
            shifted[1, pl.ds(r0 + 2, CONV_ROWS)] = v
            shifted[0, pl.ds(r0 + 2, CONV_ROWS)] = from_left(flat).astype(BF16).reshape(v.shape)
            shifted[2, pl.ds(r0 + 2, CONV_ROWS)] = from_right(flat).astype(BF16).reshape(v.shape)

    def both(own, oth, r, count):
        shape = (count * width, lanes)
        return [own[pl.ds(r, count)].reshape(shape), oth[pl.ds(r, count)].reshape(shape)]

    def conv(own, oth, r0, w_ref):
        lhs = jnp.concatenate(sum((both(own, oth, r0 + 2 - kh, CONV_ROWS) for kh in range(3)), []), axis=-1)
        out = jnp.dot(lhs, w_ref[...], preferred_element_type=F32)
        return out[:, lanes:2 * lanes] + from_right(out[:, :lanes]) + from_left(out[:, 2 * lanes:])

    def kgrad(own, oth, acc):
        def piece(r, count):
            lhs = jnp.concatenate(both(own, oth, r, count), axis=-1)
            taps = [shifted[kw, pl.ds(r + kh, count)].reshape(count * width, lanes) for kh in range(3) for kw in range(3)]
            rhs = jnp.concatenate(taps, axis=-1)
            acc[...] += lax.dot_general(lhs, rhs, (((0,), (0,)), ((), ())), preferred_element_type=F32)

        @pl.loop(0, rows // GRAD_ROWS)
        def _(k):
            piece(1 + k * GRAD_ROWS, GRAD_ROWS)

        piece(halo_row, 1)

    last_block = rows // CONV_ROWS - 1

    def blocks(halo, step):
        @pl.loop(0, last_block + 1)
        def _(k):
            @pl.when(k == last_block)
            def _():
                halo.wait()

            step((k + (last_block - 2 * k) * sp) * CONV_ROWS)

    def first(img, halo):
        own, oth = g_own.at[img % 3], g_oth.at[img % 2]
        out = z_own.at[img % 2]

        def step(r0):
            d_act = conv(own, oth, r0, weights.at[1])
            live = shifted[1, pl.ds(r0 + 2, CONV_ROWS)].reshape(m_conv, lanes).astype(F32) > 0
            masked = jnp.where(live, d_act, 0.0)
            db_ref[...] += jnp.sum(masked.reshape(m_conv // 8, 8, lanes), axis=0)
            out[pl.ds(1 + r0, CONV_ROWS)] = masked.astype(BF16).reshape(CONV_ROWS, width, lanes)

        blocks(halo, step)

    def second(img, halo):
        own, oth = z_own.at[img % 2], z_oth.at[img % 2]
        skip = g_own.at[img % 3]
        slot = img % 2

        def step(r0):
            d_x = conv(own, oth, r0, weights.at[0])
            d_x = d_x + skip[pl.ds(1 + r0, CONV_ROWS)].reshape(m_conv, lanes).astype(F32)
            out_own[slot, pl.ds(r0, CONV_ROWS)] = d_x.astype(BF16).reshape(CONV_ROWS, width, lanes)

        blocks(halo, step)

    def arrive(copies):
        main, side, forward = copies
        main.wait()
        forward.start()
        side.wait()
        return forward

    def raw_copies():
        copies = []
        for idx, src in enumerate((w1_hbm, w2_hbm)):
            copies.append(pltpu.make_async_copy(src, raw_own.at[idx], raw_sem.at[idx]))
            copies.append(remote(src, raw_rem.at[idx], raw_send.at[idx], raw_recv.at[idx], partner))
        return copies

    def local_block(block):
        on_chip = chip if block < 2 else 1 - chip
        on_core = core if block % 2 == 0 else 1 - core
        return pl.multiple_of((2 * on_chip + on_core) * half, half)

    def build_weights():
        for copy in raw_copies():
            copy.wait()
        for idx in range(2):
            @pl.loop(0, 3)
            def _(kh):
                for kw in range(3):
                    taps = jnp.concatenate([raw_own[idx, kh, kw], raw_rem[idx, kh, kw]], axis=0).T
                    for block in range(4):
                        dst = pl.ds(pl.multiple_of(kh * 4 * half, half) + local_block(block), half)
                        weights[idx, dst, kw * lanes:(kw + 1) * lanes] = taps[block * half:(block + 1) * half]

    grad_rows = TAPS * half

    def collect(acc, idx):
        @pl.loop(0, TAPS)
        def _(tap):
            cols = pl.ds(pl.multiple_of(tap * lanes, lanes), lanes)
            flipped = jnp.concatenate([acc[pl.ds(local_block(block), half), cols] for block in range(4)], axis=0).T
            dst = pl.ds(pl.multiple_of(tap * half, half), half)
            part_own[idx, dst] = flipped[:half]
            part_send[idx, dst] = flipped[half:]

    def swap_part(idx):
        return remote(part_send.at[idx], part_recv.at[idx], part_sems.at[idx, 0], part_sems.at[idx, 1], partner)

    def swap_rows():
        return remote(part_own.at[1], row_recv, part_sems.at[2, 0], part_sems.at[2, 1], beside)

    def add_part(idx):
        swap_part(idx).wait()
        part_own[idx] += part_recv[idx]

    start_loads(0, 0)
    for copy in raw_copies():
        copy.start()
    steps = num + 2
    zero_row = jnp.zeros((width, lanes), BF16)
    for slot in range(3):
        g_own[slot, edge_row] = zero_row
    for slot in range(2):
        g_oth[slot, edge_row] = zero_row
        z_own[slot, edge_row] = zero_row
        z_oth[slot, edge_row] = zero_row
    for side in range(3):
        for row in (0, 1, rows + 2, rows + 3):
            shifted[side, row] = zero_row
    tail = pl.ds(grad_rows, 8)
    for idx in range(2):
        part_own[idx, tail] = jnp.zeros((8, 2 * lanes), F32)
        part_send[idx, tail] = jnp.zeros((8, 2 * lanes), F32)

    @pl.loop(0, steps)
    def _(step):
        @pl.when(step >= 1)
        def _():
            for rel in range(3):
                pl.semaphore_wait(free_sem.at[rel], 1)

        @pl.when(step + 1 < num)
        def _():
            start_loads(0, step + 1)

        @pl.when(step < num)
        def _():
            start_loads(1, step)
            wait_loads(0, step)
            dst = g_own.at[step % 3]

            @pl.loop(0, rows // CONV_ROWS)
            def _(k):
                dst[pl.ds(1 + k * CONV_ROWS, CONV_ROWS)] = dense(0, step % 2, k * CONV_ROWS, CONV_ROWS)

            for copy in g_exchange(step)[:2]:
                copy.start()

        @pl.when(step == 0)
        def _():
            build_weights()
            acc1[...] = jnp.zeros_like(acc1)
            acc2[...] = jnp.zeros_like(acc2)
            db_ref[...] = jnp.zeros_like(db_ref)

        @pl.when((step >= 1) & (step <= num))
        def _():
            img = step - 1
            start_loads(2, img)
            wait_loads(1, img)
            prepare(1, img)
            first(img, arrive(g_exchange(img)))
            for copy in z_exchange(img)[:2]:
                copy.start()
            kgrad(g_own.at[img % 3], g_oth.at[img % 2], acc2)

            @pl.when(img == num - 1)
            def _():
                collect(acc2, 1)
                part_own[1, tail, :lanes] = db_ref[...]
                part_send[1, tail, :lanes] = pltpu.roll(db_ref[...], half, 1)
                swap_part(1).start()

        @pl.when(step >= 2)
        def _():
            img = step - 2
            wait_loads(2, img)
            prepare(2, img)

            @pl.when(img >= 1)
            def _():
                finish_out(img - 1)

            @pl.when(img >= 2)
            def _():
                store_out(img - 2).wait()

            second(img, arrive(z_exchange(img)))
            swap_out(img).start()
            kgrad(z_own.at[img % 2], z_oth.at[img % 2], acc1)

            @pl.when(img == num - 2)
            def _():
                add_part(1)
                swap_rows().start()

        @pl.when(step + 1 < steps)
        def _():
            for rel, peer in enumerate(peers):
                pl.semaphore_signal(free_sem.at[rel], inc=1, device_id=peer, device_id_type=MESH)

    collect(acc1, 0)
    swap_part(0).start()
    finish_out(num - 1)
    swap_rows().wait()
    dw2_ref[...] = part_own[1] + row_recv[...]
    add_part(0)
    dw1_ref[...] = part_own[0, :grad_rows]
    store_out(num - 2).wait()
    store_out(num - 1).wait()


def unpack(num, packed_hbm, out_hbm, packed, out, load_sem, store_sem):
    core = lax.axis_index("tp") % 2
    depth, half = packed.shape[0], out.shape[-1]

    def load(i):
        slot = i % depth
        return pltpu.make_async_copy(packed_hbm.at[i], packed.at[slot], load_sem.at[slot])

    def stores(i):
        slot = i % depth
        return [pltpu.make_async_copy(out.at[slot, side], out_hbm.at[side, i], store_sem.at[slot, side]) for side in range(2)]

    for i in range(depth):
        load(i).start()

    @pl.loop(0, num)
    def _(i):
        slot = i % depth
        load(i).wait()

        @pl.when(i >= depth)
        def _():
            for copy in stores(i - depth):
                copy.wait()

        out[slot, core] = packed[slot, ..., :half]
        out[slot, 1 - core] = packed[slot, ..., half:]
        for copy in stores(i):
            copy.start()

        @pl.when(i + depth < num)
        def _():
            load(i + depth).start()

    for i in range(num - depth, num):
        for copy in stores(i):
            copy.wait()


def solution(mesh):
    def local_step(x_in, act_saved, w_one, w_two, d_out):
        images, rows, width, half = x_in.shape
        num = images // 2
        lanes = 2 * half
        swap_rows = [(0, 1), (1, 0)]
        part = pltpu.VMEM((2, TAPS * half + 8, 4 * half), F32)
        pad = (rows + 2, width, lanes)
        dma = pltpu.SemaphoreType.DMA
        hbm = pl.BlockSpec(memory_space=pltpu.HBM)
        vmem = pl.BlockSpec(memory_space=pltpu.VMEM)
        packed, grad_one, grad_two = pl.pallas_call(
            lambda *refs: body(num, rows, width, *refs),
            out_shape=(
                jax.ShapeDtypeStruct((num, rows, width, lanes), BF16),
                jax.ShapeDtypeStruct((TAPS * half, 4 * half), F32),
                jax.ShapeDtypeStruct((TAPS * half + 8, 4 * half), F32),
            ),
            in_specs=[hbm] * 5,
            out_specs=[hbm, vmem, vmem],
            scratch_shapes=[
                pltpu.VMEM((4 * half, TAPS * lanes), F32),
                pltpu.VMEM((4 * half, TAPS * lanes), F32),
                pltpu.VMEM((8, lanes), F32),
                pltpu.VMEM((2,) + w_one.shape, BF16),
                pltpu.VMEM((2,) + w_one.shape, BF16),
                pltpu.VMEM((2, 3 * 4 * half, 3 * lanes), BF16),
                part, part, part,
                pltpu.VMEM((TAPS * half + 8, 4 * half), F32),
                pltpu.VMEM((3, 2, rows, width, half), BF16),
                pltpu.VMEM((3, 2, rows, width, half), BF16),
                pltpu.VMEM((3,) + pad, BF16),
                pltpu.VMEM((2,) + pad, BF16),
                pltpu.VMEM((2,) + pad, BF16),
                pltpu.VMEM((2,) + pad, BF16),
                pltpu.VMEM((3, rows + 4, width, lanes), BF16),
                pltpu.VMEM((2, rows, width, lanes), BF16),
                pltpu.VMEM((2, rows, width, lanes), BF16),
                dma((3, 2)), dma((3, 2)), dma((3, 2)),
                dma((3, 2)), dma((3, 2)), dma((3, 2)), dma((3, 2)),
                dma((2,)), dma((2,)), dma((2,)),
                dma((2,)), dma((2,)), dma((2,)), dma((3, 2)),
                pltpu.SemaphoreType.REGULAR((3,)),
            ],
            compiler_params=pltpu.CompilerParams(collective_id=0, has_side_effects=True, vmem_limit_bytes=60 * 1024 * 1024),
        )(x_in, act_saved, d_out, w_one, w_two)

        depth = 8
        d_x = pl.pallas_call(
            lambda *refs: unpack(num, *refs),
            out_shape=jax.ShapeDtypeStruct((2, num, rows, width, half), BF16),
            in_specs=[hbm],
            out_specs=hbm,
            scratch_shapes=[
                pltpu.VMEM((depth, rows, width, lanes), BF16),
                pltpu.VMEM((depth, 2, rows, width, half), BF16),
                dma((depth,)), dma((depth, 2)),
            ],
            cost_estimate=pl.CostEstimate(flops=10**10, bytes_accessed=5 * 10**7, transcendentals=0),
        )(packed).reshape(x_in.shape)

        grad_one = grad_one + lax.ppermute(grad_one, "sp", swap_rows)
        bias = jnp.sum(grad_two[TAPS * half:, :half], axis=0)
        grad_two = grad_two[:TAPS * half]
        return d_x, grad_one.reshape(w_one.shape), grad_two.reshape(w_two.shape), bias

    act_spec = P("dp", "sp", None, "tp")
    kern_spec = P(None, None, "tp", None)
    grad_spec = P("dp", None, "tp", None)
    return jax.shard_map(local_step, mesh=mesh, in_specs=(act_spec, act_spec, kern_spec, kern_spec, act_spec), out_specs=(act_spec, grad_spec, grad_spec, P(("dp", "tp"))), check_vma=False)
```

```python
import jax
import jax.numpy as jnp
from jax import lax
from jax.experimental import pallas as pl
from jax.experimental.pallas import tpu as pltpu
from jax.sharding import PartitionSpec as P

MESH = pl.DeviceIdType.MESH
F32, BF16 = jnp.float32, jnp.bfloat16
TAPS = 9
CONV_ROWS = 16
GRAD_ROWS = 32


def body(num, rows, width, x_hbm, a_hbm, y_hbm, w1_hbm, w2_hbm, dx_hbm, dw1_hbm, dw2_hbm,
         acc1, acc2, db_ref, raw_own, raw_rem, weights, part_own, part_send, part_recv, row_recv, nat_own, nat_rem, g_own, g_oth, z_own, z_oth, shifted, out_own, out_rem,
         load_sem, push_send, push_recv, g_send, g_recv, z_send, z_recv, out_sem, out_send, out_recv, raw_sem, raw_send, raw_recv, part_sems, free_sem):
    dp, sp, tp = lax.axis_index("dp"), lax.axis_index("sp"), lax.axis_index("tp")
    core, chip = tp % 2, tp // 2
    partner = (dp, sp, tp + 1 - 2 * core)
    across = (dp, sp, (tp + 2) % 4)
    beside = (dp, 1 - sp, tp)
    peers = (partner, across, beside)
    half = 64
    lanes = 2 * half
    edge_row = (rows + 1) * sp
    halo_row = (rows + 1) * (1 - sp)
    halo_src = rows - (rows - 1) * sp
    m_conv = CONV_ROWS * width
    m_grad = GRAD_ROWS * width

    barrier = pltpu.get_barrier_semaphore()
    for peer in peers:
        pl.semaphore_signal(barrier, inc=1, device_id=peer, device_id_type=MESH)
    pl.semaphore_wait(barrier, 3)

    def remote(src, dst, send, recv, peer):
        return pltpu.make_async_remote_copy(src_ref=src, dst_ref=dst, send_sem=send, recv_sem=recv, device_id=peer, device_id_type=MESH)

    sources = (y_hbm, a_hbm, x_hbm)

    def loads(kind, img):
        slot = img % 2
        local = pltpu.make_async_copy(sources[kind].at[core * num + img], nat_own.at[kind, slot], load_sem.at[kind, slot])
        push = remote(sources[kind].at[(1 - core) * num + img], nat_rem.at[kind, slot], push_send.at[kind, slot], push_recv.at[kind, slot], partner)
        return local, push

    def start_loads(kind, img):
        for copy in loads(kind, img):
            copy.start()

    def wait_loads(kind, img):
        for copy in loads(kind, img):
            copy.wait()

    def exchange(own, own_slot, oth, oth_slot, send, recv, sem_slot):
        return (
            remote(own.at[own_slot, pl.ds(1, rows)], oth.at[oth_slot, pl.ds(1, rows)], send.at[0, sem_slot], recv.at[0, sem_slot], across),
            remote(own.at[own_slot, halo_src], own.at[own_slot, edge_row], send.at[1, sem_slot], recv.at[1, sem_slot], beside),
            remote(oth.at[oth_slot, halo_src], oth.at[oth_slot, edge_row], send.at[2, sem_slot], recv.at[2, sem_slot], beside),
        )

    def g_exchange(img):
        return exchange(g_own, img % 3, g_oth, img % 2, g_send, g_recv, img % 2)

    def z_exchange(img):
        return exchange(z_own, img % 2, z_oth, img % 2, z_send, z_recv, img % 2)

    def swap_out(img):
        slot = img % 2
        return remote(out_own.at[slot], out_rem.at[slot], out_send.at[slot], out_recv.at[slot], partner)

    def store_out(img):
        return pltpu.make_async_copy(out_own.at[img % 2], dx_hbm.at[img], out_sem.at[img % 2])

    def finish_out(img):
        slot = img % 2
        swap_out(img).wait()

        @pl.loop(0, rows // CONV_ROWS)
        def _(k):
            block = pl.ds(k * CONV_ROWS, CONV_ROWS)
            lane = lax.broadcasted_iota(jnp.int32, (CONV_ROWS, width, lanes), 2)
            out_own[slot, block] = jnp.where(lane < half, out_own[slot, block], out_rem[slot, block])

        store_out(img).start()

    def dense(kind, slot, r0, count):
        mine = nat_own[kind, slot, pl.ds(r0, count)]
        theirs = nat_rem[kind, slot, pl.ds(r0, count)]
        return jnp.concatenate([mine, theirs], axis=-1)

    col = lax.broadcasted_iota(jnp.int32, (m_conv, lanes), 0) % width
    at_first = col == 0
    at_last = col == width - 1

    def from_right(v):
        return jnp.where(at_last, 0.0, pltpu.roll(v, m_conv - 1, 0))

    def from_left(v):
        return jnp.where(at_first, 0.0, pltpu.roll(v, 1, 0))

    def prepare(kind, img):
        @pl.loop(0, rows // CONV_ROWS)
        def _(k):
            r0 = k * CONV_ROWS
            v = dense(kind, img % 2, r0, CONV_ROWS)
            flat = v.reshape(m_conv, lanes).astype(F32)
            shifted[1, pl.ds(r0 + 2, CONV_ROWS)] = v
            shifted[0, pl.ds(r0 + 2, CONV_ROWS)] = from_left(flat).astype(BF16).reshape(v.shape)
            shifted[2, pl.ds(r0 + 2, CONV_ROWS)] = from_right(flat).astype(BF16).reshape(v.shape)

    def both(own, oth, r, count):
        shape = (count * width, lanes)
        return [own[pl.ds(r, count)].reshape(shape), oth[pl.ds(r, count)].reshape(shape)]

    def conv(own, oth, r0, w_ref):
        lhs = jnp.concatenate(sum((both(own, oth, r0 + 2 - kh, CONV_ROWS) for kh in range(3)), []), axis=-1)
        out = jnp.dot(lhs, w_ref[...], preferred_element_type=F32)
        return out[:, lanes:2 * lanes] + from_right(out[:, :lanes]) + from_left(out[:, 2 * lanes:])

    def kgrad(own, oth, acc):
        def piece(r, count):
            lhs = jnp.concatenate(both(own, oth, r, count), axis=-1)
            taps = [shifted[kw, pl.ds(r + kh, count)].reshape(count * width, lanes) for kh in range(3) for kw in range(3)]
            rhs = jnp.concatenate(taps, axis=-1)
            acc[...] += lax.dot_general(lhs, rhs, (((0,), (0,)), ((), ())), preferred_element_type=F32)

        def inner():
            @pl.loop(0, rows // GRAD_ROWS)
            def _(k):
                piece(1 + k * GRAD_ROWS, GRAD_ROWS)

        return inner, lambda: piece(halo_row, 1)

    last_block = rows // CONV_ROWS - 1

    def blocks(halo, step):
        @pl.loop(0, last_block + 1)
        def _(k):
            @pl.when(k == last_block)
            def _():
                halo.wait()

            step((k + (last_block - 2 * k) * sp) * CONV_ROWS)

    def first(img, halo):
        own, oth = g_own.at[img % 3], g_oth.at[img % 2]
        out = z_own.at[img % 2]

        def step(r0):
            d_act = conv(own, oth, r0, weights.at[1])
            live = shifted[1, pl.ds(r0 + 2, CONV_ROWS)].reshape(m_conv, lanes).astype(F32) > 0
            masked = jnp.where(live, d_act, 0.0)
            db_ref[...] += jnp.sum(masked.reshape(m_conv // 8, 8, lanes), axis=0)
            out[pl.ds(1 + r0, CONV_ROWS)] = masked.astype(BF16).reshape(CONV_ROWS, width, lanes)

        blocks(halo, step)

    def second(img, halo):
        own, oth = z_own.at[img % 2], z_oth.at[img % 2]
        skip = g_own.at[img % 3]
        slot = img % 2

        def step(r0):
            d_x = conv(own, oth, r0, weights.at[0])
            d_x = d_x + skip[pl.ds(1 + r0, CONV_ROWS)].reshape(m_conv, lanes).astype(F32)
            out_own[slot, pl.ds(r0, CONV_ROWS)] = d_x.astype(BF16).reshape(CONV_ROWS, width, lanes)

        blocks(halo, step)

    def arrive(copies):
        main, side, forward = copies
        main.wait()
        forward.start()
        side.wait()
        return forward

    def raw_copies():
        copies = []
        for idx, src in enumerate((w1_hbm, w2_hbm)):
            copies.append(pltpu.make_async_copy(src, raw_own.at[idx], raw_sem.at[idx]))
            copies.append(remote(src, raw_rem.at[idx], raw_send.at[idx], raw_recv.at[idx], partner))
        return copies

    def local_block(block):
        on_chip = chip if block < 2 else 1 - chip
        on_core = core if block % 2 == 0 else 1 - core
        return pl.multiple_of((2 * on_chip + on_core) * half, half)

    def build_weights():
        for copy in raw_copies():
            copy.wait()
        for idx in range(2):
            @pl.loop(0, 3)
            def _(kh):
                for kw in range(3):
                    taps = jnp.concatenate([raw_own[idx, kh, kw], raw_rem[idx, kh, kw]], axis=0).T
                    for block in range(4):
                        dst = pl.ds(pl.multiple_of(kh * 4 * half, half) + local_block(block), half)
                        weights[idx, dst, kw * lanes:(kw + 1) * lanes] = taps[block * half:(block + 1) * half]

    grad_rows = TAPS * half

    def collect(acc, idx):
        @pl.loop(0, TAPS)
        def _(tap):
            cols = pl.ds(pl.multiple_of(tap * lanes, lanes), lanes)
            flipped = jnp.concatenate([acc[pl.ds(local_block(block), half), cols] for block in range(4)], axis=0).T
            dst = pl.ds(pl.multiple_of(tap * half, half), half)
            part_own[idx, dst] = flipped[:half]
            part_send[idx, dst] = flipped[half:]

    def swap_part(idx):
        return remote(part_send.at[idx], part_recv.at[idx], part_sems.at[idx, 0], part_sems.at[idx, 1], partner)

    def swap_rows():
        return remote(part_own.at[1], row_recv, part_sems.at[2, 0], part_sems.at[2, 1], beside)

    def add_part(idx):
        swap_part(idx).wait()
        part_own[idx] += part_recv[idx]

    start_loads(0, 0)
    for copy in raw_copies():
        copy.start()
    steps = num + 2
    zero_row = jnp.zeros((width, lanes), BF16)
    for slot in range(3):
        g_own[slot, edge_row] = zero_row
    for slot in range(2):
        g_oth[slot, edge_row] = zero_row
        z_own[slot, edge_row] = zero_row
        z_oth[slot, edge_row] = zero_row
    for side in range(3):
        for row in (0, 1, rows + 2, rows + 3):
            shifted[side, row] = zero_row
    tail = pl.ds(grad_rows, 8)
    for idx in range(2):
        part_own[idx, tail] = jnp.zeros((8, 2 * lanes), F32)
        part_send[idx, tail] = jnp.zeros((8, 2 * lanes), F32)

    @pl.loop(0, steps)
    def _(step):
        @pl.when(step >= 1)
        def _():
            for rel in range(3):
                pl.semaphore_wait(free_sem.at[rel], 1)

        @pl.when(step + 1 < num)
        def _():
            start_loads(0, step + 1)

        @pl.when(step < num)
        def _():
            start_loads(1, step)
            wait_loads(0, step)
            dst = g_own.at[step % 3]

            @pl.loop(0, rows // CONV_ROWS)
            def _(k):
                dst[pl.ds(1 + k * CONV_ROWS, CONV_ROWS)] = dense(0, step % 2, k * CONV_ROWS, CONV_ROWS)

            for copy in g_exchange(step)[:2]:
                copy.start()

        @pl.when(step == 0)
        def _():
            build_weights()
            acc1[...] = jnp.zeros_like(acc1)
            acc2[...] = jnp.zeros_like(acc2)
            db_ref[...] = jnp.zeros_like(db_ref)

        @pl.when((step >= 1) & (step <= num))
        def _():
            img = step - 1
            start_loads(2, img)
            wait_loads(1, img)
            prepare(1, img)
            first(img, arrive(g_exchange(img)))
            for copy in z_exchange(img)[:2]:
                copy.start()
            for part in kgrad(g_own.at[img % 3], g_oth.at[img % 2], acc2):
                part()

            @pl.when(img == num - 1)
            def _():
                collect(acc2, 1)
                part_own[1, tail, :lanes] = db_ref[...]
                part_send[1, tail, :lanes] = pltpu.roll(db_ref[...], half, 1)
                swap_part(1).start()

        @pl.when(step >= 2)
        def _():
            img = step - 2
            wait_loads(2, img)
            prepare(2, img)

            @pl.when(img >= 1)
            def _():
                finish_out(img - 1)

            @pl.when(img >= 2)
            def _():
                store_out(img - 2).wait()

            @pl.when(img == num - 2)
            def _():
                add_part(1)
                swap_rows().start()

            halo = arrive(z_exchange(img))
            inner, outer = kgrad(z_own.at[img % 2], z_oth.at[img % 2], acc1)
            inner()
            second(img, halo)
            swap_out(img).start()
            outer()

        @pl.when(step + 1 < steps)
        def _():
            for rel, peer in enumerate(peers):
                pl.semaphore_signal(free_sem.at[rel], inc=1, device_id=peer, device_id_type=MESH)

    collect(acc1, 0)
    swap_part(0).start()
    finish_out(num - 1)
    swap_rows().wait()
    part_own[1] += row_recv[...]
    second_grad = pltpu.make_async_copy(part_own.at[1], dw2_hbm, raw_sem.at[1])
    second_grad.start()
    add_part(0)
    first_grad = pltpu.make_async_copy(part_own.at[0, pl.ds(0, grad_rows)], dw1_hbm, raw_sem.at[0])
    first_grad.start()
    store_out(num - 2).wait()
    store_out(num - 1).wait()
    second_grad.wait()
    first_grad.wait()


def unpack(num, packed_hbm, grad_hbm, out_hbm, grad_out, bias_out, packed, out, grad, bias, load_sem, store_sem, grad_sem):
    core = lax.axis_index("tp") % 2
    depth, half = packed.shape[0], out.shape[-1]

    def load(i):
        slot = i % depth
        return pltpu.make_async_copy(packed_hbm.at[i], packed.at[slot], load_sem.at[slot])

    def stores(i):
        slot = i % depth
        return [pltpu.make_async_copy(out.at[slot, side], out_hbm.at[side, i], store_sem.at[slot, side]) for side in range(2)]

    load_grad = pltpu.make_async_copy(grad_hbm, grad, grad_sem.at[0])
    store_grad = pltpu.make_async_copy(grad.at[pl.ds(0, TAPS * half)], grad_out, grad_sem.at[0])
    store_bias = pltpu.make_async_copy(bias, bias_out, grad_sem.at[1])
    for i in range(depth):
        load(i).start()
    load_grad.start()

    @pl.loop(0, num)
    def _(i):
        slot = i % depth
        load(i).wait()

        @pl.when(i == depth)
        def _():
            load_grad.wait()
            store_grad.start()
            bias[...] = jnp.sum(grad[TAPS * half:, :half], axis=0, keepdims=True)
            store_bias.start()

        @pl.when(i >= depth)
        def _():
            for copy in stores(i - depth):
                copy.wait()

        out[slot, core] = packed[slot, ..., :half]
        out[slot, 1 - core] = packed[slot, ..., half:]
        for copy in stores(i):
            copy.start()

        @pl.when(i + depth < num)
        def _():
            load(i + depth).start()

    for i in range(num - depth, num):
        for copy in stores(i):
            copy.wait()
    store_grad.wait()
    store_bias.wait()


def solution(mesh):
    def local_step(x_in, act_saved, w_one, w_two, d_out):
        images, rows, width, half = x_in.shape
        num = images // 2
        lanes = 2 * half
        swap_rows = [(0, 1), (1, 0)]
        part = pltpu.VMEM((2, TAPS * half + 8, 4 * half), F32)
        pad = (rows + 2, width, lanes)
        dma = pltpu.SemaphoreType.DMA
        hbm = pl.BlockSpec(memory_space=pltpu.HBM)
        packed, grad_one, grad_two = pl.pallas_call(
            lambda *refs: body(num, rows, width, *refs),
            out_shape=(
                jax.ShapeDtypeStruct((num, rows, width, lanes), BF16),
                jax.ShapeDtypeStruct((TAPS * half, 4 * half), F32),
                jax.ShapeDtypeStruct((TAPS * half + 8, 4 * half), F32),
            ),
            in_specs=[hbm] * 5,
            out_specs=[hbm] * 3,
            scratch_shapes=[
                pltpu.VMEM((4 * half, TAPS * lanes), F32),
                pltpu.VMEM((4 * half, TAPS * lanes), F32),
                pltpu.VMEM((8, lanes), F32),
                pltpu.VMEM((2,) + w_one.shape, BF16),
                pltpu.VMEM((2,) + w_one.shape, BF16),
                pltpu.VMEM((2, 3 * 4 * half, 3 * lanes), BF16),
                part, part, part,
                pltpu.VMEM((TAPS * half + 8, 4 * half), F32),
                pltpu.VMEM((3, 2, rows, width, half), BF16),
                pltpu.VMEM((3, 2, rows, width, half), BF16),
                pltpu.VMEM((3,) + pad, BF16),
                pltpu.VMEM((2,) + pad, BF16),
                pltpu.VMEM((2,) + pad, BF16),
                pltpu.VMEM((2,) + pad, BF16),
                pltpu.VMEM((3, rows + 4, width, lanes), BF16),
                pltpu.VMEM((2, rows, width, lanes), BF16),
                pltpu.VMEM((2, rows, width, lanes), BF16),
                dma((3, 2)), dma((3, 2)), dma((3, 2)),
                dma((3, 2)), dma((3, 2)), dma((3, 2)), dma((3, 2)),
                dma((2,)), dma((2,)), dma((2,)),
                dma((2,)), dma((2,)), dma((2,)), dma((3, 2)),
                pltpu.SemaphoreType.REGULAR((3,)),
            ],
            compiler_params=pltpu.CompilerParams(collective_id=0, has_side_effects=True, vmem_limit_bytes=60 * 1024 * 1024),
        )(x_in, act_saved, d_out, w_one, w_two)

        depth = 8
        d_x, grad_two, bias = pl.pallas_call(
            lambda *refs: unpack(num, *refs),
            out_shape=(
                jax.ShapeDtypeStruct((2, num, rows, width, half), BF16),
                jax.ShapeDtypeStruct((TAPS * half, 4 * half), F32),
                jax.ShapeDtypeStruct((1, half), F32),
            ),
            in_specs=[hbm] * 2,
            out_specs=[hbm] * 3,
            scratch_shapes=[
                pltpu.VMEM((depth, rows, width, lanes), BF16),
                pltpu.VMEM((depth, 2, rows, width, half), BF16),
                pltpu.VMEM((TAPS * half + 8, 4 * half), F32),
                pltpu.VMEM((1, half), F32),
                dma((depth,)), dma((depth, 2)), dma((2,)),
            ],
            cost_estimate=pl.CostEstimate(flops=10**10, bytes_accessed=5 * 10**7, transcendentals=0),
        )(packed, grad_two)
        grad_one = grad_one + lax.ppermute(grad_one, "sp", swap_rows)
        return d_x.reshape(x_in.shape), grad_one.reshape(w_one.shape), grad_two.reshape(w_two.shape), bias.reshape(half)

    act_spec = P("dp", "sp", None, "tp")
    kern_spec = P(None, None, "tp", None)
    grad_spec = P("dp", None, "tp", None)
    return jax.shard_map(local_step, mesh=mesh, in_specs=(act_spec, act_spec, kern_spec, kern_spec, act_spec), out_specs=(act_spec, grad_spec, grad_spec, P(("dp", "tp"))), check_vma=False)
```

```python
import jax
import jax.numpy as jnp
from jax import lax
from jax.experimental import pallas as pl
from jax.experimental.pallas import tpu as pltpu
from jax.sharding import PartitionSpec as P

MESH = pl.DeviceIdType.MESH
F32, BF16 = jnp.float32, jnp.bfloat16
TAPS = 9
CONV_ROWS = 16
GRAD_ROWS = 32


def body(num, rows, width, x_hbm, a_hbm, y_hbm, w1_ref, w2_ref, packed, dw1_ref, dw2_ref,
         acc1, acc2, db_ref, raw_rem, weights, part_own, part_send, part_recv, row_recv, nat_own, nat_rem, g_own, g_oth, z_own, z_oth, shifted, out_own, out_rem,
         load_sem, push_send, push_recv, g_send, g_recv, z_send, z_recv, out_send, out_recv, raw_send, raw_recv, part_sems, free_sem):
    dp, sp, tp = lax.axis_index("dp"), lax.axis_index("sp"), lax.axis_index("tp")
    core, chip = tp % 2, tp // 2
    partner = (dp, sp, tp + 1 - 2 * core)
    across = (dp, sp, (tp + 2) % 4)
    beside = (dp, 1 - sp, tp)
    peers = (partner, across, beside)
    half = 64
    lanes = 2 * half
    edge_row = (rows + 1) * sp
    halo_row = (rows + 1) * (1 - sp)
    halo_src = rows - (rows - 1) * sp
    m_conv = CONV_ROWS * width
    m_grad = GRAD_ROWS * width

    barrier = pltpu.get_barrier_semaphore()
    for peer in peers:
        pl.semaphore_signal(barrier, inc=1, device_id=peer, device_id_type=MESH)
    pl.semaphore_wait(barrier, 3)

    def remote(src, dst, send, recv, peer):
        return pltpu.make_async_remote_copy(src_ref=src, dst_ref=dst, send_sem=send, recv_sem=recv, device_id=peer, device_id_type=MESH)

    sources = (y_hbm, a_hbm, x_hbm)

    def loads(kind, img):
        slot = img % 2
        local = pltpu.make_async_copy(sources[kind].at[core * num + img], nat_own.at[kind, slot], load_sem.at[kind, slot])
        push = remote(sources[kind].at[(1 - core) * num + img], nat_rem.at[kind, slot], push_send.at[kind, slot], push_recv.at[kind, slot], partner)
        return local, push

    def start_loads(kind, img):
        for copy in loads(kind, img):
            copy.start()

    def wait_loads(kind, img):
        for copy in loads(kind, img):
            copy.wait()

    def exchange(own, own_slot, oth, oth_slot, send, recv, sem_slot):
        return (
            remote(own.at[own_slot, pl.ds(1, rows)], oth.at[oth_slot, pl.ds(1, rows)], send.at[0, sem_slot], recv.at[0, sem_slot], across),
            remote(own.at[own_slot, halo_src], own.at[own_slot, edge_row], send.at[1, sem_slot], recv.at[1, sem_slot], beside),
            remote(oth.at[oth_slot, halo_src], oth.at[oth_slot, edge_row], send.at[2, sem_slot], recv.at[2, sem_slot], beside),
        )

    def g_exchange(img):
        return exchange(g_own, img % 3, g_oth, img % 2, g_send, g_recv, img % 2)

    def z_exchange(img):
        return exchange(z_own, img % 2, z_oth, img % 2, z_send, z_recv, img % 2)

    def swap_out(img):
        slot = img % 2
        return remote(out_own.at[slot], out_rem.at[slot], out_send.at[slot], out_recv.at[slot], partner)

    def finish_out(img):
        slot = img % 2
        swap_out(img).wait()

        @pl.loop(0, rows // CONV_ROWS)
        def _(k):
            block = pl.ds(k * CONV_ROWS, CONV_ROWS)
            lane = lax.broadcasted_iota(jnp.int32, (CONV_ROWS, width, lanes), 2)
            packed[img, block] = jnp.where(lane < half, out_own[slot, block], out_rem[slot, block])

    def dense(kind, slot, r0, count):
        mine = nat_own[kind, slot, pl.ds(r0, count)]
        theirs = nat_rem[kind, slot, pl.ds(r0, count)]
        return jnp.concatenate([mine, theirs], axis=-1)

    col = lax.broadcasted_iota(jnp.int32, (m_conv, lanes), 0) % width
    at_first = col == 0
    at_last = col == width - 1

    def from_right(v):
        return jnp.where(at_last, 0.0, pltpu.roll(v, m_conv - 1, 0))

    def from_left(v):
        return jnp.where(at_first, 0.0, pltpu.roll(v, 1, 0))

    def prepare(kind, img):
        @pl.loop(0, rows // CONV_ROWS)
        def _(k):
            r0 = k * CONV_ROWS
            v = dense(kind, img % 2, r0, CONV_ROWS)
            flat = v.reshape(m_conv, lanes).astype(F32)
            shifted[1, pl.ds(r0 + 2, CONV_ROWS)] = v
            shifted[0, pl.ds(r0 + 2, CONV_ROWS)] = from_left(flat).astype(BF16).reshape(v.shape)
            shifted[2, pl.ds(r0 + 2, CONV_ROWS)] = from_right(flat).astype(BF16).reshape(v.shape)

    def both(own, oth, r, count):
        shape = (count * width, lanes)
        return [own[pl.ds(r, count)].reshape(shape), oth[pl.ds(r, count)].reshape(shape)]

    def conv(own, oth, r0, w_ref):
        lhs = jnp.concatenate(sum((both(own, oth, r0 + 2 - kh, CONV_ROWS) for kh in range(3)), []), axis=-1)
        out = jnp.dot(lhs, w_ref[...], preferred_element_type=F32)
        return out[:, lanes:2 * lanes] + from_right(out[:, :lanes]) + from_left(out[:, 2 * lanes:])

    def kgrad(own, oth, acc):
        def piece(r, count):
            lhs = jnp.concatenate(both(own, oth, r, count), axis=-1)
            taps = [shifted[kw, pl.ds(r + kh, count)].reshape(count * width, lanes) for kh in range(3) for kw in range(3)]
            rhs = jnp.concatenate(taps, axis=-1)
            acc[...] += lax.dot_general(lhs, rhs, (((0,), (0,)), ((), ())), preferred_element_type=F32)

        def inner():
            @pl.loop(0, rows // GRAD_ROWS)
            def _(k):
                piece(1 + k * GRAD_ROWS, GRAD_ROWS)

        return inner, lambda: piece(halo_row, 1)

    last_block = rows // CONV_ROWS - 1

    def blocks(halo, step):
        @pl.loop(0, last_block + 1)
        def _(k):
            @pl.when(k == last_block)
            def _():
                halo.wait()

            step((k + (last_block - 2 * k) * sp) * CONV_ROWS)

    def first(img, halo):
        own, oth = g_own.at[img % 3], g_oth.at[img % 2]
        out = z_own.at[img % 2]

        def step(r0):
            d_act = conv(own, oth, r0, weights.at[1])
            live = shifted[1, pl.ds(r0 + 2, CONV_ROWS)].reshape(m_conv, lanes).astype(F32) > 0
            masked = jnp.where(live, d_act, 0.0)
            db_ref[...] += jnp.sum(masked.reshape(m_conv // 8, 8, lanes), axis=0)
            out[pl.ds(1 + r0, CONV_ROWS)] = masked.astype(BF16).reshape(CONV_ROWS, width, lanes)

        blocks(halo, step)

    def second(img, halo):
        own, oth = z_own.at[img % 2], z_oth.at[img % 2]
        skip = g_own.at[img % 3]
        slot = img % 2

        def step(r0):
            d_x = conv(own, oth, r0, weights.at[0])
            d_x = d_x + skip[pl.ds(1 + r0, CONV_ROWS)].reshape(m_conv, lanes).astype(F32)
            out_own[slot, pl.ds(r0, CONV_ROWS)] = d_x.astype(BF16).reshape(CONV_ROWS, width, lanes)

        blocks(halo, step)

    def arrive(copies):
        main, side, forward = copies
        main.wait()
        forward.start()
        side.wait()
        return forward

    raw = (w1_ref, w2_ref)

    def swap_raw(idx):
        return remote(raw[idx], raw_rem.at[idx], raw_send.at[idx], raw_recv.at[idx], partner)

    def local_block(block):
        on_chip = chip if block < 2 else 1 - chip
        on_core = core if block % 2 == 0 else 1 - core
        return pl.multiple_of((2 * on_chip + on_core) * half, half)

    def build_weights():
        for idx in range(2):
            swap_raw(idx).wait()

            @pl.loop(0, 3)
            def _(kh):
                for kw in range(3):
                    taps = jnp.concatenate([raw[idx][kh, kw], raw_rem[idx, kh, kw]], axis=0).T
                    for block in range(4):
                        dst = pl.ds(pl.multiple_of(kh * 4 * half, half) + local_block(block), half)
                        weights[idx, dst, kw * lanes:(kw + 1) * lanes] = taps[block * half:(block + 1) * half]

    grad_rows = TAPS * half

    def collect(acc, idx):
        @pl.loop(0, TAPS)
        def _(tap):
            cols = pl.ds(pl.multiple_of(tap * lanes, lanes), lanes)
            flipped = jnp.concatenate([acc[pl.ds(local_block(block), half), cols] for block in range(4)], axis=0).T
            dst = pl.ds(pl.multiple_of(tap * half, half), half)
            part_own[idx, dst] = flipped[:half]
            part_send[idx, dst] = flipped[half:]

    def swap_part(idx):
        return remote(part_send.at[idx], part_recv.at[idx], part_sems.at[idx, 0], part_sems.at[idx, 1], partner)

    def swap_rows():
        return remote(part_own.at[1], row_recv, part_sems.at[2, 0], part_sems.at[2, 1], beside)

    def add_part(idx):
        swap_part(idx).wait()
        part_own[idx] += part_recv[idx]

    start_loads(0, 0)
    for idx in range(2):
        swap_raw(idx).start()
    steps = num + 2
    zero_row = jnp.zeros((width, lanes), BF16)
    for slot in range(3):
        g_own[slot, edge_row] = zero_row
    for slot in range(2):
        g_oth[slot, edge_row] = zero_row
        z_own[slot, edge_row] = zero_row
        z_oth[slot, edge_row] = zero_row
    for side in range(3):
        for row in (0, 1, rows + 2, rows + 3):
            shifted[side, row] = zero_row
    tail = pl.ds(grad_rows, 8)
    for idx in range(2):
        part_own[idx, tail] = jnp.zeros((8, 2 * lanes), F32)
        part_send[idx, tail] = jnp.zeros((8, 2 * lanes), F32)

    @pl.loop(0, steps)
    def _(step):
        @pl.when(step >= 1)
        def _():
            for rel in range(3):
                pl.semaphore_wait(free_sem.at[rel], 1)

        @pl.when(step + 1 < num)
        def _():
            start_loads(0, step + 1)

        @pl.when(step < num)
        def _():
            start_loads(1, step)
            wait_loads(0, step)
            dst = g_own.at[step % 3]

            @pl.loop(0, rows // CONV_ROWS)
            def _(k):
                dst[pl.ds(1 + k * CONV_ROWS, CONV_ROWS)] = dense(0, step % 2, k * CONV_ROWS, CONV_ROWS)

            for copy in g_exchange(step)[:2]:
                copy.start()

        @pl.when(step == 0)
        def _():
            build_weights()
            acc1[...] = jnp.zeros_like(acc1)
            acc2[...] = jnp.zeros_like(acc2)
            db_ref[...] = jnp.zeros_like(db_ref)

        @pl.when((step >= 1) & (step <= num))
        def _():
            img = step - 1
            start_loads(2, img)
            wait_loads(1, img)
            prepare(1, img)
            first(img, arrive(g_exchange(img)))
            for copy in z_exchange(img)[:2]:
                copy.start()
            for part in kgrad(g_own.at[img % 3], g_oth.at[img % 2], acc2):
                part()

            @pl.when(img == num - 1)
            def _():
                collect(acc2, 1)
                part_own[1, tail, :lanes] = db_ref[...]
                part_send[1, tail, :lanes] = pltpu.roll(db_ref[...], half, 1)
                swap_part(1).start()

        @pl.when(step >= 2)
        def _():
            img = step - 2
            wait_loads(2, img)
            prepare(2, img)

            @pl.when(img >= 1)
            def _():
                finish_out(img - 1)

            @pl.when(img == num - 2)
            def _():
                add_part(1)
                swap_rows().start()

            halo = arrive(z_exchange(img))
            inner, outer = kgrad(z_own.at[img % 2], z_oth.at[img % 2], acc1)
            inner()
            second(img, halo)
            swap_out(img).start()
            outer()

        @pl.when(step + 1 < steps)
        def _():
            for rel, peer in enumerate(peers):
                pl.semaphore_signal(free_sem.at[rel], inc=1, device_id=peer, device_id_type=MESH)

    collect(acc1, 0)
    swap_part(0).start()
    finish_out(num - 1)
    swap_rows().wait()
    dw2_ref[...] = part_own[1] + row_recv[...]
    swap_part(0).wait()
    inside = pl.ds(0, grad_rows)
    dw1_ref[...] = part_own[0, inside] + part_recv[0, inside]


def unpack(num, packed, grad, out_hbm, grad_out, bias_out, out, bias, store_sem, grad_sem):
    core = lax.axis_index("tp") % 2
    depth, half = out.shape[0], out.shape[-1]

    def stores(i):
        slot = i % depth
        return [pltpu.make_async_copy(out.at[slot, side], out_hbm.at[side, i], store_sem.at[slot, side]) for side in range(2)]

    store_grad = pltpu.make_async_copy(grad.at[pl.ds(0, TAPS * half)], grad_out, grad_sem.at[0])
    store_bias = pltpu.make_async_copy(bias, bias_out, grad_sem.at[1])
    store_grad.start()
    bias[...] = jnp.sum(grad[TAPS * half:, :half], axis=0, keepdims=True)
    store_bias.start()

    @pl.loop(0, num)
    def _(i):
        slot = i % depth

        @pl.when(i >= depth)
        def _():
            for copy in stores(i - depth):
                copy.wait()

        out[slot, core] = packed[i, ..., :half]
        out[slot, 1 - core] = packed[i, ..., half:]
        for copy in stores(i):
            copy.start()

    for i in range(num - depth, num):
        for copy in stores(i):
            copy.wait()
    store_grad.wait()
    store_bias.wait()


def solution(mesh):
    def local_step(x_in, act_saved, w_one, w_two, d_out):
        images, rows, width, half = x_in.shape
        num = images // 2
        lanes = 2 * half
        swap_rows = [(0, 1), (1, 0)]
        part = pltpu.VMEM((2, TAPS * half + 8, 4 * half), F32)
        pad = (rows + 2, width, lanes)
        dma = pltpu.SemaphoreType.DMA
        hbm = pl.BlockSpec(memory_space=pltpu.HBM)
        vmem = pl.BlockSpec(memory_space=pltpu.VMEM)
        packed, grad_one, grad_two = pl.pallas_call(
            lambda *refs: body(num, rows, width, *refs),
            out_shape=(
                jax.ShapeDtypeStruct((num, rows, width, lanes), BF16),
                jax.ShapeDtypeStruct((TAPS * half, 4 * half), F32),
                jax.ShapeDtypeStruct((TAPS * half + 8, 4 * half), F32),
            ),
            in_specs=[hbm] * 3 + [vmem] * 2,
            out_specs=[vmem] * 3,
            scratch_shapes=[
                pltpu.VMEM((4 * half, TAPS * lanes), F32),
                pltpu.VMEM((4 * half, TAPS * lanes), F32),
                pltpu.VMEM((8, lanes), F32),
                pltpu.VMEM((2,) + w_one.shape, BF16),
                pltpu.VMEM((2, 3 * 4 * half, 3 * lanes), BF16),
                part, part, part,
                pltpu.VMEM((TAPS * half + 8, 4 * half), F32),
                pltpu.VMEM((3, 2, rows, width, half), BF16),
                pltpu.VMEM((3, 2, rows, width, half), BF16),
                pltpu.VMEM((3,) + pad, BF16),
                pltpu.VMEM((2,) + pad, BF16),
                pltpu.VMEM((2,) + pad, BF16),
                pltpu.VMEM((2,) + pad, BF16),
                pltpu.VMEM((3, rows + 4, width, lanes), BF16),
                pltpu.VMEM((2, rows, width, lanes), BF16),
                pltpu.VMEM((2, rows, width, lanes), BF16),
                dma((3, 2)), dma((3, 2)), dma((3, 2)),
                dma((3, 2)), dma((3, 2)), dma((3, 2)), dma((3, 2)),
                dma((2,)), dma((2,)),
                dma((2,)), dma((2,)), dma((3, 2)),
                pltpu.SemaphoreType.REGULAR((3,)),
            ],
            compiler_params=pltpu.CompilerParams(collective_id=0, has_side_effects=True, vmem_limit_bytes=30 * 1024 * 1024),
        )(x_in, act_saved, d_out, w_one, w_two)

        depth = 8
        d_x, grad_two, bias = pl.pallas_call(
            lambda *refs: unpack(num, *refs),
            out_shape=(
                jax.ShapeDtypeStruct((2, num, rows, width, half), BF16),
                jax.ShapeDtypeStruct((TAPS * half, 4 * half), F32),
                jax.ShapeDtypeStruct((1, half), F32),
            ),
            in_specs=[vmem] * 2,
            out_specs=[hbm] * 3,
            scratch_shapes=[
                pltpu.VMEM((depth, 2, rows, width, half), BF16),
                pltpu.VMEM((1, half), F32),
                dma((depth, 2)), dma((2,)),
            ],
            compiler_params=pltpu.CompilerParams(vmem_limit_bytes=14 * 1024 * 1024),
            cost_estimate=pl.CostEstimate(flops=10**10, bytes_accessed=5 * 10**7, transcendentals=0),
        )(packed, grad_two)
        grad_one = grad_one + lax.ppermute(grad_one, "sp", swap_rows)
        return d_x.reshape(x_in.shape), grad_one.reshape(w_one.shape), grad_two.reshape(w_two.shape), bias.reshape(half)

    act_spec = P("dp", "sp", None, "tp")
    kern_spec = P(None, None, "tp", None)
    grad_spec = P("dp", None, "tp", None)
    return jax.shard_map(local_step, mesh=mesh, in_specs=(act_spec, act_spec, kern_spec, kern_spec, act_spec), out_specs=(act_spec, grad_spec, grad_spec, P(("dp", "tp"))), check_vma=False)
```

```python
import jax
import jax.numpy as jnp
from jax import lax
from jax.experimental import pallas as pl
from jax.experimental.pallas import tpu as pltpu
from jax.sharding import PartitionSpec as P

MESH = pl.DeviceIdType.MESH
F32, BF16 = jnp.float32, jnp.bfloat16
TAPS = 9
CONV_ROWS = 16
GRAD_ROWS = 32


def body(num, rows, width, x_hbm, a_hbm, y_hbm, w1_ref, w2_ref, packed, dw1_ref, dw1_rest_ref, dw2_ref,
         acc1, acc2, db_ref, raw_rem, weights, part_own, part_send, part_recv, row_recv, nat_own, nat_rem, g_own, g_oth, z_own, z_oth, shifted, out_own, out_rem,
         load_sem, push_send, push_recv, g_send, g_recv, z_send, z_recv, out_send, out_recv, raw_send, raw_recv, part_sems, free_sem):
    dp, sp, tp = lax.axis_index("dp"), lax.axis_index("sp"), lax.axis_index("tp")
    core, chip = tp % 2, tp // 2
    partner = (dp, sp, tp + 1 - 2 * core)
    across = (dp, sp, (tp + 2) % 4)
    beside = (dp, 1 - sp, tp)
    peers = (partner, across, beside)
    half = 64
    lanes = 2 * half
    edge_row = (rows + 1) * sp
    halo_row = (rows + 1) * (1 - sp)
    halo_src = rows - (rows - 1) * sp
    m_conv = CONV_ROWS * width
    m_grad = GRAD_ROWS * width

    barrier = pltpu.get_barrier_semaphore()
    for peer in peers:
        pl.semaphore_signal(barrier, inc=1, device_id=peer, device_id_type=MESH)
    pl.semaphore_wait(barrier, 3)

    def remote(src, dst, send, recv, peer):
        return pltpu.make_async_remote_copy(src_ref=src, dst_ref=dst, send_sem=send, recv_sem=recv, device_id=peer, device_id_type=MESH)

    sources = (y_hbm, a_hbm, x_hbm)

    def loads(kind, img):
        slot = img % 2
        local = pltpu.make_async_copy(sources[kind].at[core * num + img], nat_own.at[kind, slot], load_sem.at[kind, slot])
        push = remote(sources[kind].at[(1 - core) * num + img], nat_rem.at[kind, slot], push_send.at[kind, slot], push_recv.at[kind, slot], partner)
        return local, push

    def start_loads(kind, img):
        for copy in loads(kind, img):
            copy.start()

    def wait_loads(kind, img):
        for copy in loads(kind, img):
            copy.wait()

    def exchange(own, own_slot, oth, oth_slot, send, recv, sem_slot):
        return (
            remote(own.at[own_slot, pl.ds(1, rows)], oth.at[oth_slot, pl.ds(1, rows)], send.at[0, sem_slot], recv.at[0, sem_slot], across),
            remote(own.at[own_slot, halo_src], own.at[own_slot, edge_row], send.at[1, sem_slot], recv.at[1, sem_slot], beside),
            remote(oth.at[oth_slot, halo_src], oth.at[oth_slot, edge_row], send.at[2, sem_slot], recv.at[2, sem_slot], beside),
        )

    def g_exchange(img):
        return exchange(g_own, img % 3, g_oth, img % 2, g_send, g_recv, img % 2)

    def z_exchange(img):
        return exchange(z_own, img % 2, z_oth, img % 2, z_send, z_recv, img % 2)

    def swap_out(img):
        slot = img % 2
        return remote(out_own.at[slot], out_rem.at[slot], out_send.at[slot], out_recv.at[slot], partner)

    def finish_out(img):
        slot = img % 2
        swap_out(img).wait()

        @pl.loop(0, rows // CONV_ROWS)
        def _(k):
            block = pl.ds(k * CONV_ROWS, CONV_ROWS)
            lane = lax.broadcasted_iota(jnp.int32, (CONV_ROWS, width, lanes), 2)
            packed[img, block] = jnp.where(lane < half, out_own[slot, block], out_rem[slot, block])

    def dense(kind, slot, r0, count):
        mine = nat_own[kind, slot, pl.ds(r0, count)]
        theirs = nat_rem[kind, slot, pl.ds(r0, count)]
        return jnp.concatenate([mine, theirs], axis=-1)

    col = lax.broadcasted_iota(jnp.int32, (m_conv, lanes), 0) % width
    at_first = col == 0
    at_last = col == width - 1

    def from_right(v):
        return jnp.where(at_last, 0.0, pltpu.roll(v, m_conv - 1, 0))

    def from_left(v):
        return jnp.where(at_first, 0.0, pltpu.roll(v, 1, 0))

    def prepare(kind, img):
        @pl.loop(0, rows // CONV_ROWS)
        def _(k):
            r0 = k * CONV_ROWS
            v = dense(kind, img % 2, r0, CONV_ROWS)
            flat = v.reshape(m_conv, lanes).astype(F32)
            shifted[1, pl.ds(r0 + 2, CONV_ROWS)] = v
            shifted[0, pl.ds(r0 + 2, CONV_ROWS)] = from_left(flat).astype(BF16).reshape(v.shape)
            shifted[2, pl.ds(r0 + 2, CONV_ROWS)] = from_right(flat).astype(BF16).reshape(v.shape)

    def both(own, oth, r, count):
        shape = (count * width, lanes)
        return [own[pl.ds(r, count)].reshape(shape), oth[pl.ds(r, count)].reshape(shape)]

    def conv(own, oth, r0, w_ref):
        lhs = jnp.concatenate(sum((both(own, oth, r0 + 2 - kh, CONV_ROWS) for kh in range(3)), []), axis=-1)
        out = jnp.dot(lhs, w_ref[...], preferred_element_type=F32)
        return out[:, lanes:2 * lanes] + from_right(out[:, :lanes]) + from_left(out[:, 2 * lanes:])

    def kgrad(sources, acc, first_row):
        dst = pl.ds(first_row, lanes * len(sources))

        def piece(r, count):
            shape = (count * width, lanes)
            lhs = jnp.concatenate([src[pl.ds(r, count)].reshape(shape) for src in sources], axis=-1)
            taps = [shifted[kw, pl.ds(r + kh, count)].reshape(shape) for kh in range(3) for kw in range(3)]
            rhs = jnp.concatenate(taps, axis=-1)
            acc[dst] += lax.dot_general(lhs, rhs, (((0,), (0,)), ((), ())), preferred_element_type=F32)

        def inner():
            @pl.loop(0, rows // GRAD_ROWS)
            def _(k):
                piece(1 + k * GRAD_ROWS, GRAD_ROWS)

        return inner, lambda: piece(halo_row, 1)

    last_block = rows // CONV_ROWS - 1

    def blocks(halo, step):
        @pl.loop(0, last_block + 1)
        def _(k):
            @pl.when(k == last_block)
            def _():
                halo.wait()

            step((k + (last_block - 2 * k) * sp) * CONV_ROWS)

    def first(img, halo):
        own, oth = g_own.at[img % 3], g_oth.at[img % 2]
        out = z_own.at[img % 2]

        def step(r0):
            d_act = conv(own, oth, r0, weights.at[1])
            live = shifted[1, pl.ds(r0 + 2, CONV_ROWS)].reshape(m_conv, lanes).astype(F32) > 0
            masked = jnp.where(live, d_act, 0.0)
            db_ref[...] += jnp.sum(masked.reshape(m_conv // 8, 8, lanes), axis=0)
            out[pl.ds(1 + r0, CONV_ROWS)] = masked.astype(BF16).reshape(CONV_ROWS, width, lanes)

        blocks(halo, step)

    def second(img, halo):
        own, oth = z_own.at[img % 2], z_oth.at[img % 2]
        skip = g_own.at[img % 3]
        slot = img % 2

        def step(r0):
            d_x = conv(own, oth, r0, weights.at[0])
            d_x = d_x + skip[pl.ds(1 + r0, CONV_ROWS)].reshape(m_conv, lanes).astype(F32)
            out_own[slot, pl.ds(r0, CONV_ROWS)] = d_x.astype(BF16).reshape(CONV_ROWS, width, lanes)

        blocks(halo, step)

    def arrive(copies):
        main, _, forward = copies
        main.wait()
        forward.start()
        return forward

    raw = (w1_ref, w2_ref)

    def swap_raw(idx):
        return remote(raw[idx], raw_rem.at[idx], raw_send.at[idx], raw_recv.at[idx], partner)

    def local_block(block):
        on_chip = chip if block < 2 else 1 - chip
        on_core = core if block % 2 == 0 else 1 - core
        return pl.multiple_of((2 * on_chip + on_core) * half, half)

    def build_weights():
        for idx in range(2):
            swap_raw(idx).wait()

            @pl.loop(0, 3)
            def _(kh):
                for kw in range(3):
                    taps = jnp.concatenate([raw[idx][kh, kw], raw_rem[idx, kh, kw]], axis=0).T
                    for block in range(4):
                        dst = pl.ds(pl.multiple_of(kh * 4 * half, half) + local_block(block), half)
                        weights[idx, dst, kw * lanes:(kw + 1) * lanes] = taps[block * half:(block + 1) * half]

    grad_rows = TAPS * half

    def collect(acc, side, idx):
        @pl.loop(0, TAPS)
        def _(tap):
            cols = pl.ds(pl.multiple_of(tap * lanes, lanes), lanes)
            firsts = (core, 1 - core)
            pieces = [acc[pl.ds(pl.multiple_of(side * lanes + first * half, half), half), cols] for first in firsts]
            flipped = jnp.concatenate(pieces, axis=0).T
            dst = pl.ds(pl.multiple_of(tap * half, half), half)
            part_own[idx, dst] = flipped[:half]
            part_send[idx, dst] = flipped[half:]

    def swap_part(lo, count):
        which = pl.ds(lo, count)
        return remote(part_send.at[which], part_recv.at[which], part_sems.at[0, lo], part_sems.at[1, lo], partner)

    def swap_rows(lo, count):
        which = pl.ds(lo, count)
        return remote(part_own.at[which], row_recv.at[which], part_sems.at[2, lo], part_sems.at[3, lo], beside)

    def add_part(lo, count):
        swap_part(lo, count).wait()
        which = pl.ds(lo, count)
        part_own[which] += part_recv[which]

    start_loads(0, 0)
    for idx in range(2):
        swap_raw(idx).start()
    steps = num + 2
    zero_row = jnp.zeros((width, lanes), BF16)
    for slot in range(3):
        g_own[slot, edge_row] = zero_row
    for slot in range(2):
        g_oth[slot, edge_row] = zero_row
        z_own[slot, edge_row] = zero_row
        z_oth[slot, edge_row] = zero_row
    for side in range(3):
        for row in (0, 1, rows + 2, rows + 3):
            shifted[side, row] = zero_row
    tail = pl.ds(grad_rows, 8)
    for idx in range(4):
        part_own[idx, tail] = jnp.zeros((8, lanes), F32)
        part_send[idx, tail] = jnp.zeros((8, lanes), F32)

    @pl.loop(0, steps)
    def _(step):
        @pl.when(step >= 1)
        def _():
            for rel in range(3):
                pl.semaphore_wait(free_sem.at[rel], 1)

        @pl.when(step + 1 < num)
        def _():
            start_loads(0, step + 1)

        @pl.when(step < num)
        def _():
            start_loads(1, step)
            wait_loads(0, step)
            dst = g_own.at[step % 3]

            @pl.loop(0, rows // CONV_ROWS)
            def _(k):
                dst[pl.ds(1 + k * CONV_ROWS, CONV_ROWS)] = dense(0, step % 2, k * CONV_ROWS, CONV_ROWS)

            for copy in g_exchange(step)[:2]:
                copy.start()

        @pl.when(step == 0)
        def _():
            build_weights()
            acc1[...] = jnp.zeros_like(acc1)
            acc2[...] = jnp.zeros_like(acc2)
            db_ref[...] = jnp.zeros_like(db_ref)

        @pl.when((step >= 1) & (step <= num))
        def _():
            img = step - 1
            start_loads(2, img)
            wait_loads(1, img)
            prepare(1, img)
            copies = g_exchange(img)
            halo = arrive(copies)
            copies[1].wait()
            first(img, halo)
            for copy in z_exchange(img)[:2]:
                copy.start()
            for part in kgrad((g_own.at[img % 3], g_oth.at[img % 2]), acc2, 0):
                part()

            @pl.when(img == num - 1)
            def _():
                collect(acc2, 0, 2)
                collect(acc2, 1, 3)
                part_own[2, tail] = db_ref[...]
                part_send[2, tail] = pltpu.roll(db_ref[...], half, 1)
                swap_part(2, 2).start()

        @pl.when(step >= 2)
        def _():
            img = step - 2
            wait_loads(2, img)
            prepare(2, img)

            @pl.when(img >= 1)
            def _():
                finish_out(img - 1)

            @pl.when(img == num - 2)
            def _():
                add_part(2, 2)
                swap_rows(2, 2).start()

            copies = z_exchange(img)
            copies[1].wait()
            for part in kgrad((z_own.at[img % 2],), acc1, 0):
                part()

            @pl.when(img == num - 1)
            def _():
                collect(acc1, 0, 0)
                swap_part(0, 1).start()
                add_part(0, 1)
                swap_rows(0, 1).start()

            halo = arrive(copies)
            inner, outer = kgrad((z_oth.at[img % 2],), acc1, lanes)
            inner()
            second(img, halo)
            swap_out(img).start()
            outer()

        @pl.when(step + 1 < steps)
        def _():
            for rel, peer in enumerate(peers):
                pl.semaphore_signal(free_sem.at[rel], inc=1, device_id=peer, device_id_type=MESH)

    collect(acc1, 1, 1)
    swap_part(1, 1).start()
    finish_out(num - 1)
    swap_rows(2, 2).wait()
    dw2_ref[...] = part_own[pl.ds(2, 2)] + row_recv[pl.ds(2, 2)]
    swap_rows(0, 1).wait()
    inside = pl.ds(0, grad_rows)
    dw1_ref[...] = part_own[0, inside] + row_recv[0, inside]
    swap_part(1, 1).wait()
    dw1_rest_ref[...] = part_own[1, inside] + part_recv[1, inside]


def unpack(num, packed, grad, out_hbm, grad_out, bias_out, out, bias, store_sem, grad_sem):
    core = lax.axis_index("tp") % 2
    depth, half = out.shape[0], out.shape[-1]

    def stores(i):
        slot = i % depth
        return [pltpu.make_async_copy(out.at[slot, side], out_hbm.at[side, i], store_sem.at[slot, side]) for side in range(2)]

    chip = lax.axis_index("tp") // 2
    inside = pl.ds(0, TAPS * half)
    store_grads = [
        pltpu.make_async_copy(grad.at[side, inside], grad_out.at[:, pl.ds(tile * 2 * half, 2 * half)], grad_sem.at[tile])
        for tile, side in enumerate((chip, 1 - chip))
    ]
    store_bias = pltpu.make_async_copy(bias, bias_out, grad_sem.at[2])
    for copy in store_grads:
        copy.start()
    bias[...] = jnp.sum(grad[0, TAPS * half:, :half], axis=0, keepdims=True)
    store_bias.start()

    @pl.loop(0, num)
    def _(i):
        slot = i % depth

        @pl.when(i >= depth)
        def _():
            for copy in stores(i - depth):
                copy.wait()

        out[slot, core] = packed[i, ..., :half]
        out[slot, 1 - core] = packed[i, ..., half:]
        for copy in stores(i):
            copy.start()

    for i in range(num - depth, num):
        for copy in stores(i):
            copy.wait()
    for copy in store_grads + [store_bias]:
        copy.wait()


def solution(mesh):
    def local_step(x_in, act_saved, w_one, w_two, d_out):
        images, rows, width, half = x_in.shape
        num = images // 2
        lanes = 2 * half
        swap_rows = [(0, 1), (1, 0)]
        part = pltpu.VMEM((4, TAPS * half + 8, lanes), F32)
        pad = (rows + 2, width, lanes)
        dma = pltpu.SemaphoreType.DMA
        hbm = pl.BlockSpec(memory_space=pltpu.HBM)
        vmem = pl.BlockSpec(memory_space=pltpu.VMEM)
        packed, near, far, grad_two = pl.pallas_call(
            lambda *refs: body(num, rows, width, *refs),
            out_shape=(
                jax.ShapeDtypeStruct((num, rows, width, lanes), BF16),
                jax.ShapeDtypeStruct((TAPS * half, lanes), F32),
                jax.ShapeDtypeStruct((TAPS * half, lanes), F32),
                jax.ShapeDtypeStruct((2, TAPS * half + 8, lanes), F32),
            ),
            in_specs=[hbm] * 3 + [vmem] * 2,
            out_specs=[vmem] * 4,
            scratch_shapes=[
                pltpu.VMEM((4 * half, TAPS * lanes), F32),
                pltpu.VMEM((4 * half, TAPS * lanes), F32),
                pltpu.VMEM((8, lanes), F32),
                pltpu.VMEM((2,) + w_one.shape, BF16),
                pltpu.VMEM((2, 3 * 4 * half, 3 * lanes), BF16),
                part, part, part, part,
                pltpu.VMEM((3, 2, rows, width, half), BF16),
                pltpu.VMEM((3, 2, rows, width, half), BF16),
                pltpu.VMEM((3,) + pad, BF16),
                pltpu.VMEM((2,) + pad, BF16),
                pltpu.VMEM((2,) + pad, BF16),
                pltpu.VMEM((2,) + pad, BF16),
                pltpu.VMEM((3, rows + 4, width, lanes), BF16),
                pltpu.VMEM((2, rows, width, lanes), BF16),
                pltpu.VMEM((2, rows, width, lanes), BF16),
                dma((3, 2)), dma((3, 2)), dma((3, 2)),
                dma((3, 2)), dma((3, 2)), dma((3, 2)), dma((3, 2)),
                dma((2,)), dma((2,)),
                dma((2,)), dma((2,)), dma((4, 4)),
                pltpu.SemaphoreType.REGULAR((3,)),
            ],
            compiler_params=pltpu.CompilerParams(collective_id=0, has_side_effects=True, vmem_limit_bytes=30 * 1024 * 1024),
        )(x_in, act_saved, d_out, w_one, w_two)

        depth = 8
        d_x, grad_two, bias = pl.pallas_call(
            lambda *refs: unpack(num, *refs),
            out_shape=(
                jax.ShapeDtypeStruct((2, num, rows, width, half), BF16),
                jax.ShapeDtypeStruct((TAPS * half, 4 * half), F32),
                jax.ShapeDtypeStruct((1, half), F32),
            ),
            in_specs=[vmem] * 2,
            out_specs=[hbm] * 3,
            scratch_shapes=[
                pltpu.VMEM((depth, 2, rows, width, half), BF16),
                pltpu.VMEM((1, half), F32),
                dma((depth, 2)), dma((3,)),
            ],
            compiler_params=pltpu.CompilerParams(vmem_limit_bytes=14 * 1024 * 1024),
            cost_estimate=pl.CostEstimate(flops=10**10, bytes_accessed=5 * 10**7, transcendentals=0),
        )(packed, grad_two)
        far = far + lax.ppermute(far, "sp", swap_rows)
        on_left = lax.axis_index("tp") < 2
        grad_one = jnp.concatenate([jnp.where(on_left, near, far), jnp.where(on_left, far, near)], axis=1)
        return d_x.reshape(x_in.shape), grad_one.reshape(w_one.shape), grad_two.reshape(w_two.shape), bias.reshape(half)

    act_spec = P("dp", "sp", None, "tp")
    kern_spec = P(None, None, "tp", None)
    grad_spec = P("dp", None, "tp", None)
    return jax.shard_map(local_step, mesh=mesh, in_specs=(act_spec, act_spec, kern_spec, kern_spec, act_spec), out_specs=(act_spec, grad_spec, grad_spec, P(("dp", "tp"))), check_vma=False)
```

```python
import jax
import jax.numpy as jnp
from jax import lax
from jax.experimental import pallas as pl
from jax.experimental.pallas import tpu as pltpu
from jax.sharding import PartitionSpec as P

MESH = pl.DeviceIdType.MESH
F32, BF16 = jnp.float32, jnp.bfloat16
TAPS = 9
CONV_ROWS = 16
GRAD_ROWS = 32


def body(num, rows, width, x_hbm, a_hbm, y_hbm, w1_ref, w2_ref, packed, dw1_ref, dw1_rest_ref, dw2_ref,
         acc1, acc2, db_ref, raw_rem, weights, part_own, part_send, part_recv, row_recv, nat_own, nat_rem, g_own, g_oth, z_own, z_oth, shifted, out_own, out_rem,
         load_sem, push_send, push_recv, g_send, g_recv, z_send, z_recv, out_send, out_recv, raw_send, raw_recv, part_sems, free_sem):
    dp, sp, tp = lax.axis_index("dp"), lax.axis_index("sp"), lax.axis_index("tp")
    core, chip = tp % 2, tp // 2
    partner = (dp, sp, tp + 1 - 2 * core)
    across = (dp, sp, (tp + 2) % 4)
    beside = (dp, 1 - sp, tp)
    peers = (partner, across, beside)
    half = 64
    lanes = 2 * half
    edge_row = (rows + 1) * sp
    halo_row = (rows + 1) * (1 - sp)
    halo_src = rows - (rows - 1) * sp
    m_conv = CONV_ROWS * width
    m_grad = GRAD_ROWS * width

    barrier = pltpu.get_barrier_semaphore()
    for peer in peers:
        pl.semaphore_signal(barrier, inc=1, device_id=peer, device_id_type=MESH)
    pl.semaphore_wait(barrier, 3)

    def remote(src, dst, send, recv, peer):
        return pltpu.make_async_remote_copy(src_ref=src, dst_ref=dst, send_sem=send, recv_sem=recv, device_id=peer, device_id_type=MESH)

    sources = (y_hbm, a_hbm, x_hbm)

    def loads(kind, img):
        slot = img % 2
        local = pltpu.make_async_copy(sources[kind].at[core * num + img], nat_own.at[kind, slot], load_sem.at[kind, slot])
        push = remote(sources[kind].at[(1 - core) * num + img], nat_rem.at[kind, slot], push_send.at[kind, slot], push_recv.at[kind, slot], partner)
        return local, push

    def start_loads(kind, img):
        for copy in loads(kind, img):
            copy.start()

    def wait_loads(kind, img):
        for copy in loads(kind, img):
            copy.wait()

    def exchange(own, own_slot, oth, oth_slot, send, recv, sem_slot):
        return (
            remote(own.at[own_slot, pl.ds(1, rows)], oth.at[oth_slot, pl.ds(1, rows)], send.at[0, sem_slot], recv.at[0, sem_slot], across),
            remote(own.at[own_slot, halo_src], own.at[own_slot, edge_row], send.at[1, sem_slot], recv.at[1, sem_slot], beside),
            remote(oth.at[oth_slot, halo_src], oth.at[oth_slot, edge_row], send.at[2, sem_slot], recv.at[2, sem_slot], beside),
        )

    def g_exchange(img):
        return exchange(g_own, img % 3, g_oth, img % 2, g_send, g_recv, img % 2)

    def z_exchange(img):
        return exchange(z_own, img % 2, z_oth, img % 2, z_send, z_recv, img % 2)

    def swap_out(img):
        slot = img % 2
        return remote(out_own.at[slot], out_rem.at[slot], out_send.at[slot], out_recv.at[slot], partner)

    def finish_out(img):
        slot = img % 2
        swap_out(img).wait()

        @pl.loop(0, rows // CONV_ROWS)
        def _(k):
            block = pl.ds(k * CONV_ROWS, CONV_ROWS)
            lane = lax.broadcasted_iota(jnp.int32, (CONV_ROWS, width, lanes), 2)
            packed[img, block] = jnp.where(lane < half, out_own[slot, block], out_rem[slot, block])

    def dense(kind, slot, r0, count):
        mine = nat_own[kind, slot, pl.ds(r0, count)]
        theirs = nat_rem[kind, slot, pl.ds(r0, count)]
        return jnp.concatenate([mine, theirs], axis=-1)

    col = lax.broadcasted_iota(jnp.int32, (m_conv, lanes), 0) % width
    at_first = col == 0
    at_last = col == width - 1

    def from_right(v):
        return jnp.where(at_last, 0.0, pltpu.roll(v, m_conv - 1, 0))

    def from_left(v):
        return jnp.where(at_first, 0.0, pltpu.roll(v, 1, 0))

    def prepare(kind, img):
        @pl.loop(0, rows // CONV_ROWS)
        def _(k):
            r0 = k * CONV_ROWS
            v = dense(kind, img % 2, r0, CONV_ROWS)
            flat = v.reshape(m_conv, lanes).astype(F32)
            shifted[1, pl.ds(r0 + 2, CONV_ROWS)] = v
            shifted[0, pl.ds(r0 + 2, CONV_ROWS)] = from_left(flat).astype(BF16).reshape(v.shape)
            shifted[2, pl.ds(r0 + 2, CONV_ROWS)] = from_right(flat).astype(BF16).reshape(v.shape)

    def both(own, oth, r, count):
        shape = (count * width, lanes)
        return [own[pl.ds(r, count)].reshape(shape), oth[pl.ds(r, count)].reshape(shape)]

    def conv(own, oth, r0, w_ref):
        lhs = jnp.concatenate(sum((both(own, oth, r0 + 2 - kh, CONV_ROWS) for kh in range(3)), []), axis=-1)
        out = jnp.dot(lhs, w_ref[...], preferred_element_type=F32)
        return out[:, lanes:2 * lanes] + from_right(out[:, :lanes]) + from_left(out[:, 2 * lanes:])

    def kgrad(sources, acc, first_row):
        dst = pl.ds(first_row, lanes * len(sources))

        def piece(r, count):
            shape = (count * width, lanes)
            lhs = jnp.concatenate([src[pl.ds(r, count)].reshape(shape) for src in sources], axis=-1)
            taps = [shifted[kw, pl.ds(r + kh, count)].reshape(shape) for kh in range(3) for kw in range(3)]
            rhs = jnp.concatenate(taps, axis=-1)
            acc[dst] += lax.dot_general(lhs, rhs, (((0,), (0,)), ((), ())), preferred_element_type=F32)

        def inner():
            @pl.loop(0, rows // GRAD_ROWS)
            def _(k):
                piece(1 + k * GRAD_ROWS, GRAD_ROWS)

        return inner, lambda: piece(halo_row, 1)

    last_block = rows // CONV_ROWS - 1

    def blocks(halo, step):
        @pl.loop(0, last_block + 1)
        def _(k):
            @pl.when(k == last_block)
            def _():
                halo.wait()

            step((k + (last_block - 2 * k) * sp) * CONV_ROWS)

    def first(img, halo):
        own, oth = g_own.at[img % 3], g_oth.at[img % 2]
        out = z_own.at[img % 2]

        def step(r0):
            d_act = conv(own, oth, r0, weights.at[1])
            live = shifted[1, pl.ds(r0 + 2, CONV_ROWS)].reshape(m_conv, lanes).astype(F32) > 0
            masked = jnp.where(live, d_act, 0.0)
            db_ref[...] += jnp.sum(masked.reshape(m_conv // 8, 8, lanes), axis=0)
            out[pl.ds(1 + r0, CONV_ROWS)] = masked.astype(BF16).reshape(CONV_ROWS, width, lanes)

        blocks(halo, step)

    def second(img, halo):
        own, oth = z_own.at[img % 2], z_oth.at[img % 2]
        skip = g_own.at[img % 3]
        slot = img % 2

        def step(r0):
            d_x = conv(own, oth, r0, weights.at[0])
            d_x = d_x + skip[pl.ds(1 + r0, CONV_ROWS)].reshape(m_conv, lanes).astype(F32)
            out_own[slot, pl.ds(r0, CONV_ROWS)] = d_x.astype(BF16).reshape(CONV_ROWS, width, lanes)

        blocks(halo, step)

    def arrive(copies):
        main, _, forward = copies
        main.wait()
        forward.start()
        return forward

    raw = (w1_ref, w2_ref)

    def swap_raw(idx):
        return remote(raw[idx], raw_rem.at[idx], raw_send.at[idx], raw_recv.at[idx], partner)

    def local_block(block):
        on_chip = chip if block < 2 else 1 - chip
        on_core = core if block % 2 == 0 else 1 - core
        return pl.multiple_of((2 * on_chip + on_core) * half, half)

    def build_weights():
        for idx in range(2):
            swap_raw(idx).wait()

            @pl.loop(0, 3)
            def _(kh):
                for kw in range(3):
                    taps = jnp.concatenate([raw[idx][kh, kw], raw_rem[idx, kh, kw]], axis=0).T
                    for block in range(4):
                        dst = pl.ds(pl.multiple_of(kh * 4 * half, half) + local_block(block), half)
                        weights[idx, dst, kw * lanes:(kw + 1) * lanes] = taps[block * half:(block + 1) * half]

    grad_rows = TAPS * half

    def collect(acc, side, idx):
        @pl.loop(0, TAPS)
        def _(tap):
            cols = pl.ds(pl.multiple_of(tap * lanes, lanes), lanes)
            firsts = (core, 1 - core)
            pieces = [acc[pl.ds(pl.multiple_of(side * lanes + first * half, half), half), cols] for first in firsts]
            flipped = jnp.concatenate(pieces, axis=0).T
            dst = pl.ds(pl.multiple_of(tap * half, half), half)
            part_own[idx, dst] = flipped[:half]
            part_send[idx, dst] = flipped[half:]

    def swap_part(lo, count):
        which = pl.ds(lo, count)
        return remote(part_send.at[which], part_recv.at[which], part_sems.at[0, lo], part_sems.at[1, lo], partner)

    third = grad_rows // 3
    whole = grad_rows + 8
    row_pieces = ((2, 0, whole), (3, 0, whole), (0, 0, third), (0, third, third), (0, 2 * third, third))

    def swap_rows(piece):
        idx, start, count = row_pieces[piece]
        which = pl.ds(start, count)
        return remote(part_own.at[idx, which], row_recv.at[idx, which], part_sems.at[2, piece], part_sems.at[3, piece], beside)

    def add_part(lo, count):
        swap_part(lo, count).wait()
        which = pl.ds(lo, count)
        part_own[which] += part_recv[which]

    start_loads(0, 0)
    for idx in range(2):
        swap_raw(idx).start()
    steps = num + 2
    zero_row = jnp.zeros((width, lanes), BF16)
    for slot in range(3):
        g_own[slot, edge_row] = zero_row
    for slot in range(2):
        g_oth[slot, edge_row] = zero_row
        z_own[slot, edge_row] = zero_row
        z_oth[slot, edge_row] = zero_row
    for side in range(3):
        for row in (0, 1, rows + 2, rows + 3):
            shifted[side, row] = zero_row
    tail = pl.ds(grad_rows, 8)
    for idx in range(4):
        part_own[idx, tail] = jnp.zeros((8, lanes), F32)
        part_send[idx, tail] = jnp.zeros((8, lanes), F32)

    @pl.loop(0, steps)
    def _(step):
        @pl.when(step >= 1)
        def _():
            for rel in range(3):
                pl.semaphore_wait(free_sem.at[rel], 1)

        @pl.when(step + 1 < num)
        def _():
            start_loads(0, step + 1)

        @pl.when(step < num)
        def _():
            start_loads(1, step)
            wait_loads(0, step)
            dst = g_own.at[step % 3]

            @pl.loop(0, rows // CONV_ROWS)
            def _(k):
                dst[pl.ds(1 + k * CONV_ROWS, CONV_ROWS)] = dense(0, step % 2, k * CONV_ROWS, CONV_ROWS)

            for copy in g_exchange(step)[:2]:
                copy.start()

        @pl.when(step == 0)
        def _():
            build_weights()
            acc1[...] = jnp.zeros_like(acc1)
            acc2[...] = jnp.zeros_like(acc2)
            db_ref[...] = jnp.zeros_like(db_ref)

        @pl.when((step >= 1) & (step <= num))
        def _():
            img = step - 1
            start_loads(2, img)
            wait_loads(1, img)
            prepare(1, img)
            copies = g_exchange(img)
            halo = arrive(copies)
            copies[1].wait()
            first(img, halo)
            for copy in z_exchange(img)[:2]:
                copy.start()
            for part in kgrad((g_own.at[img % 3], g_oth.at[img % 2]), acc2, 0):
                part()

            @pl.when(img == num - 1)
            def _():
                collect(acc2, 0, 2)
                collect(acc2, 1, 3)
                part_own[2, tail] = db_ref[...]
                part_send[2, tail] = pltpu.roll(db_ref[...], half, 1)
                swap_part(2, 2).start()

        @pl.when(step >= 2)
        def _():
            img = step - 2
            wait_loads(2, img)
            prepare(2, img)

            @pl.when(img >= 1)
            def _():
                finish_out(img - 1)

            @pl.when(img == num - 2)
            def _():
                add_part(2, 2)
                swap_rows(0).start()

            copies = z_exchange(img)
            copies[1].wait()
            for part in kgrad((z_own.at[img % 2],), acc1, 0):
                part()

            @pl.when(img == num - 1)
            def _():
                collect(acc1, 0, 0)
                swap_part(0, 1).start()
                add_part(0, 1)
                swap_rows(2).start()

            halo = arrive(copies)

            @pl.when(img == num - 2)
            def _():
                swap_rows(1).start()

            @pl.when(img == num - 1)
            def _():
                swap_rows(3).start()
                swap_rows(4).start()

            inner, outer = kgrad((z_oth.at[img % 2],), acc1, lanes)
            inner()
            second(img, halo)
            swap_out(img).start()
            outer()

        @pl.when(step + 1 < steps)
        def _():
            for rel, peer in enumerate(peers):
                pl.semaphore_signal(free_sem.at[rel], inc=1, device_id=peer, device_id_type=MESH)

    collect(acc1, 1, 1)
    swap_part(1, 1).start()
    finish_out(num - 1)
    swap_rows(0).wait()
    swap_rows(1).wait()
    dw2_ref[...] = part_own[pl.ds(2, 2)] + row_recv[pl.ds(2, 2)]
    inside = pl.ds(0, grad_rows)
    swap_part(1, 1).wait()
    dw1_rest_ref[...] = part_own[1, inside] + part_recv[1, inside]
    for piece in range(2, 5):
        swap_rows(piece).wait()
    dw1_ref[...] = part_own[0, inside] + row_recv[0, inside]


def unpack(num, packed, grad, out_hbm, grad_out, bias_out, out, bias, store_sem, grad_sem):
    core = lax.axis_index("tp") % 2
    depth, half = out.shape[0], out.shape[-1]

    def stores(i):
        slot = i % depth
        return [pltpu.make_async_copy(out.at[slot, side], out_hbm.at[side, i], store_sem.at[slot, side]) for side in range(2)]

    chip = lax.axis_index("tp") // 2
    inside = pl.ds(0, TAPS * half)
    store_grads = [
        pltpu.make_async_copy(grad.at[side, inside], grad_out.at[:, pl.ds(tile * 2 * half, 2 * half)], grad_sem.at[tile])
        for tile, side in enumerate((chip, 1 - chip))
    ]
    store_bias = pltpu.make_async_copy(bias, bias_out, grad_sem.at[2])
    for copy in store_grads:
        copy.start()
    bias[...] = jnp.sum(grad[0, TAPS * half:, :half], axis=0, keepdims=True)
    store_bias.start()

    @pl.loop(0, num)
    def _(i):
        slot = i % depth

        @pl.when(i >= depth)
        def _():
            for copy in stores(i - depth):
                copy.wait()

        out[slot, core] = packed[i, ..., :half]
        out[slot, 1 - core] = packed[i, ..., half:]
        for copy in stores(i):
            copy.start()

    for i in range(num - depth, num):
        for copy in stores(i):
            copy.wait()
    for copy in store_grads + [store_bias]:
        copy.wait()


def solution(mesh):
    def local_step(x_in, act_saved, w_one, w_two, d_out):
        images, rows, width, half = x_in.shape
        num = images // 2
        lanes = 2 * half
        swap_rows = [(0, 1), (1, 0)]
        part = pltpu.VMEM((4, TAPS * half + 8, lanes), F32)
        pad = (rows + 2, width, lanes)
        dma = pltpu.SemaphoreType.DMA
        hbm = pl.BlockSpec(memory_space=pltpu.HBM)
        vmem = pl.BlockSpec(memory_space=pltpu.VMEM)
        packed, near, far, grad_two = pl.pallas_call(
            lambda *refs: body(num, rows, width, *refs),
            out_shape=(
                jax.ShapeDtypeStruct((num, rows, width, lanes), BF16),
                jax.ShapeDtypeStruct((TAPS * half, lanes), F32),
                jax.ShapeDtypeStruct((TAPS * half, lanes), F32),
                jax.ShapeDtypeStruct((2, TAPS * half + 8, lanes), F32),
            ),
            in_specs=[hbm] * 3 + [vmem] * 2,
            out_specs=[vmem] * 4,
            scratch_shapes=[
                pltpu.VMEM((4 * half, TAPS * lanes), F32),
                pltpu.VMEM((4 * half, TAPS * lanes), F32),
                pltpu.VMEM((8, lanes), F32),
                pltpu.VMEM((2,) + w_one.shape, BF16),
                pltpu.VMEM((2, 3 * 4 * half, 3 * lanes), BF16),
                part, part, part, part,
                pltpu.VMEM((3, 2, rows, width, half), BF16),
                pltpu.VMEM((3, 2, rows, width, half), BF16),
                pltpu.VMEM((3,) + pad, BF16),
                pltpu.VMEM((2,) + pad, BF16),
                pltpu.VMEM((2,) + pad, BF16),
                pltpu.VMEM((2,) + pad, BF16),
                pltpu.VMEM((3, rows + 4, width, lanes), BF16),
                pltpu.VMEM((2, rows, width, lanes), BF16),
                pltpu.VMEM((2, rows, width, lanes), BF16),
                dma((3, 2)), dma((3, 2)), dma((3, 2)),
                dma((3, 2)), dma((3, 2)), dma((3, 2)), dma((3, 2)),
                dma((2,)), dma((2,)),
                dma((2,)), dma((2,)), dma((4, 5)),
                pltpu.SemaphoreType.REGULAR((3,)),
            ],
            compiler_params=pltpu.CompilerParams(collective_id=0, has_side_effects=True, vmem_limit_bytes=30 * 1024 * 1024),
        )(x_in, act_saved, d_out, w_one, w_two)

        depth = 8
        d_x, grad_two, bias = pl.pallas_call(
            lambda *refs: unpack(num, *refs),
            out_shape=(
                jax.ShapeDtypeStruct((2, num, rows, width, half), BF16),
                jax.ShapeDtypeStruct((TAPS * half, 4 * half), F32),
                jax.ShapeDtypeStruct((1, half), F32),
            ),
            in_specs=[vmem] * 2,
            out_specs=[hbm] * 3,
            scratch_shapes=[
                pltpu.VMEM((depth, 2, rows, width, half), BF16),
                pltpu.VMEM((1, half), F32),
                dma((depth, 2)), dma((3,)),
            ],
            compiler_params=pltpu.CompilerParams(vmem_limit_bytes=14 * 1024 * 1024),
            cost_estimate=pl.CostEstimate(flops=10**10, bytes_accessed=5 * 10**7, transcendentals=0),
        )(packed, grad_two)
        far = far + lax.ppermute(far, "sp", swap_rows)
        on_left = lax.axis_index("tp") < 2
        grad_one = jnp.concatenate([jnp.where(on_left, near, far), jnp.where(on_left, far, near)], axis=1)
        return d_x.reshape(x_in.shape), grad_one.reshape(w_one.shape), grad_two.reshape(w_two.shape), bias.reshape(half)

    act_spec = P("dp", "sp", None, "tp")
    kern_spec = P(None, None, "tp", None)
    grad_spec = P("dp", None, "tp", None)
    return jax.shard_map(local_step, mesh=mesh, in_specs=(act_spec, act_spec, kern_spec, kern_spec, act_spec), out_specs=(act_spec, grad_spec, grad_spec, P(("dp", "tp"))), check_vma=False)
```

```python
import jax
import jax.numpy as jnp
from jax import lax
from jax.experimental import pallas as pl
from jax.experimental.pallas import tpu as pltpu
from jax.sharding import PartitionSpec as P

MESH = pl.DeviceIdType.MESH
F32, BF16 = jnp.float32, jnp.bfloat16
TAPS = 9
CONV_ROWS = 16
GRAD_ROWS = 32


def body(num, rows, width, x_hbm, a_hbm, y_hbm, w1_hbm, w2_hbm, packed, dw1_ref, dw1_rest_ref, dw2_ref,
         acc1, acc2, db_ref, raw_own, raw_rem, weights, part_own, part_send, part_recv, row_recv, nat_own, nat_rem, g_own, g_oth, z_own, z_oth, shifted, out_own, out_rem,
         load_sem, push_send, push_recv, g_send, g_recv, z_send, z_recv, out_send, out_recv, raw_sem, raw_send, raw_recv, part_sems, free_sem):
    dp, sp, tp = lax.axis_index("dp"), lax.axis_index("sp"), lax.axis_index("tp")
    core, chip = tp % 2, tp // 2
    partner = (dp, sp, tp + 1 - 2 * core)
    across = (dp, sp, (tp + 2) % 4)
    beside = (dp, 1 - sp, tp)
    peers = (partner, across, beside)
    half = 64
    lanes = 2 * half
    edge_row = (rows + 1) * sp
    halo_row = (rows + 1) * (1 - sp)
    halo_src = rows - (rows - 1) * sp
    m_conv = CONV_ROWS * width
    m_grad = GRAD_ROWS * width

    barrier = pltpu.get_barrier_semaphore()
    for peer in peers:
        pl.semaphore_signal(barrier, inc=1, device_id=peer, device_id_type=MESH)
    pl.semaphore_wait(barrier, 3)

    def remote(src, dst, send, recv, peer):
        return pltpu.make_async_remote_copy(src_ref=src, dst_ref=dst, send_sem=send, recv_sem=recv, device_id=peer, device_id_type=MESH)

    sources = (y_hbm, a_hbm, x_hbm)

    def loads(kind, img):
        slot = img % 2
        local = pltpu.make_async_copy(sources[kind].at[core * num + img], nat_own.at[kind, slot], load_sem.at[kind, slot])
        push = remote(sources[kind].at[(1 - core) * num + img], nat_rem.at[kind, slot], push_send.at[kind, slot], push_recv.at[kind, slot], partner)
        return local, push

    def start_loads(kind, img):
        for copy in loads(kind, img):
            copy.start()

    def wait_loads(kind, img):
        for copy in loads(kind, img):
            copy.wait()

    def exchange(own, own_slot, oth, oth_slot, send, recv, sem_slot):
        return (
            remote(own.at[own_slot, pl.ds(1, rows)], oth.at[oth_slot, pl.ds(1, rows)], send.at[0, sem_slot], recv.at[0, sem_slot], across),
            remote(own.at[own_slot, halo_src], own.at[own_slot, edge_row], send.at[1, sem_slot], recv.at[1, sem_slot], beside),
            remote(oth.at[oth_slot, halo_src], oth.at[oth_slot, edge_row], send.at[2, sem_slot], recv.at[2, sem_slot], beside),
        )

    def g_exchange(img):
        return exchange(g_own, img % 3, g_oth, img % 2, g_send, g_recv, img % 2)

    def z_exchange(img):
        return exchange(z_own, img % 2, z_oth, img % 2, z_send, z_recv, img % 2)

    def swap_out(img):
        slot = img % 2
        return remote(out_own.at[slot], out_rem.at[slot], out_send.at[slot], out_recv.at[slot], partner)

    def finish_out(img):
        slot = img % 2
        swap_out(img).wait()

        @pl.loop(0, rows // CONV_ROWS)
        def _(k):
            block = pl.ds(k * CONV_ROWS, CONV_ROWS)
            lane = lax.broadcasted_iota(jnp.int32, (CONV_ROWS, width, lanes), 2)
            packed[img, block] = jnp.where(lane < half, out_own[slot, block], out_rem[slot, block])

    def dense(kind, slot, r0, count):
        mine = nat_own[kind, slot, pl.ds(r0, count)]
        theirs = nat_rem[kind, slot, pl.ds(r0, count)]
        return jnp.concatenate([mine, theirs], axis=-1)

    col = lax.broadcasted_iota(jnp.int32, (m_conv, lanes), 0) % width
    at_first = col == 0
    at_last = col == width - 1

    def from_right(v):
        return jnp.where(at_last, 0.0, pltpu.roll(v, m_conv - 1, 0))

    def from_left(v):
        return jnp.where(at_first, 0.0, pltpu.roll(v, 1, 0))

    def prepare(kind, img):
        @pl.loop(0, rows // CONV_ROWS)
        def _(k):
            r0 = k * CONV_ROWS
            v = dense(kind, img % 2, r0, CONV_ROWS)
            flat = v.reshape(m_conv, lanes).astype(F32)
            shifted[1, pl.ds(r0 + 2, CONV_ROWS)] = v
            shifted[0, pl.ds(r0 + 2, CONV_ROWS)] = from_left(flat).astype(BF16).reshape(v.shape)
            shifted[2, pl.ds(r0 + 2, CONV_ROWS)] = from_right(flat).astype(BF16).reshape(v.shape)

    def both(own, oth, r, count):
        shape = (count * width, lanes)
        return [own[pl.ds(r, count)].reshape(shape), oth[pl.ds(r, count)].reshape(shape)]

    def conv(own, oth, r0, w_ref):
        lhs = jnp.concatenate(sum((both(own, oth, r0 + 2 - kh, CONV_ROWS) for kh in range(3)), []), axis=-1)
        out = jnp.dot(lhs, w_ref[...], preferred_element_type=F32)
        return out[:, lanes:2 * lanes] + from_right(out[:, :lanes]) + from_left(out[:, 2 * lanes:])

    def kgrad(sources, acc, first_row):
        dst = pl.ds(first_row, lanes * len(sources))

        def piece(r, count):
            shape = (count * width, lanes)
            lhs = jnp.concatenate([src[pl.ds(r, count)].reshape(shape) for src in sources], axis=-1)
            taps = [shifted[kw, pl.ds(r + kh, count)].reshape(shape) for kh in range(3) for kw in range(3)]
            rhs = jnp.concatenate(taps, axis=-1)
            acc[dst] += lax.dot_general(lhs, rhs, (((0,), (0,)), ((), ())), preferred_element_type=F32)

        def inner():
            @pl.loop(0, rows // GRAD_ROWS)
            def _(k):
                piece(1 + k * GRAD_ROWS, GRAD_ROWS)

        return inner, lambda: piece(halo_row, 1)

    last_block = rows // CONV_ROWS - 1

    def blocks(halo, step):
        @pl.loop(0, last_block + 1)
        def _(k):
            @pl.when(k == last_block)
            def _():
                halo.wait()

            step((k + (last_block - 2 * k) * sp) * CONV_ROWS)

    def first(img, halo):
        own, oth = g_own.at[img % 3], g_oth.at[img % 2]
        out = z_own.at[img % 2]

        def step(r0):
            d_act = conv(own, oth, r0, weights.at[1])
            live = shifted[1, pl.ds(r0 + 2, CONV_ROWS)].reshape(m_conv, lanes).astype(F32) > 0
            masked = jnp.where(live, d_act, 0.0)
            db_ref[...] += jnp.sum(masked.reshape(m_conv // 8, 8, lanes), axis=0)
            out[pl.ds(1 + r0, CONV_ROWS)] = masked.astype(BF16).reshape(CONV_ROWS, width, lanes)

        blocks(halo, step)

    def second(img, halo):
        own, oth = z_own.at[img % 2], z_oth.at[img % 2]
        skip = g_own.at[img % 3]
        slot = img % 2

        def step(r0):
            d_x = conv(own, oth, r0, weights.at[0])
            d_x = d_x + skip[pl.ds(1 + r0, CONV_ROWS)].reshape(m_conv, lanes).astype(F32)
            out_own[slot, pl.ds(r0, CONV_ROWS)] = d_x.astype(BF16).reshape(CONV_ROWS, width, lanes)

        blocks(halo, step)

    def arrive(copies):
        main, _, forward = copies
        main.wait()
        forward.start()
        return forward

    raw = (w1_hbm, w2_hbm)

    def swap_raw(idx):
        return remote(raw[idx], raw_rem.at[idx], raw_send.at[idx], raw_recv.at[idx], partner)

    def load_raw(idx):
        return pltpu.make_async_copy(raw[idx], raw_own.at[idx], raw_sem.at[idx])

    def local_block(block):
        on_chip = chip if block < 2 else 1 - chip
        on_core = core if block % 2 == 0 else 1 - core
        return pl.multiple_of((2 * on_chip + on_core) * half, half)

    def build_weights():
        for idx in range(2):
            load_raw(idx).wait()
            swap_raw(idx).wait()

            @pl.loop(0, 3)
            def _(kh):
                for kw in range(3):
                    taps = jnp.concatenate([raw_own[idx, kh, kw], raw_rem[idx, kh, kw]], axis=0).T
                    for block in range(4):
                        dst = pl.ds(pl.multiple_of(kh * 4 * half, half) + local_block(block), half)
                        weights[idx, dst, kw * lanes:(kw + 1) * lanes] = taps[block * half:(block + 1) * half]

    grad_rows = TAPS * half

    def collect(acc, side, idx):
        @pl.loop(0, TAPS)
        def _(tap):
            cols = pl.ds(pl.multiple_of(tap * lanes, lanes), lanes)
            firsts = (core, 1 - core)
            pieces = [acc[pl.ds(pl.multiple_of(side * lanes + first * half, half), half), cols] for first in firsts]
            flipped = jnp.concatenate(pieces, axis=0).T
            dst = pl.ds(pl.multiple_of(tap * half, half), half)
            part_own[idx, dst] = flipped[:half]
            part_send[idx, dst] = flipped[half:]

    def swap_part(lo, count):
        which = pl.ds(lo, count)
        return remote(part_send.at[which], part_recv.at[which], part_sems.at[0, lo], part_sems.at[1, lo], partner)

    third = grad_rows // 3
    whole = grad_rows + 8
    row_pieces = ((2, 0, whole), (3, 0, whole), (0, 0, third), (0, third, third))

    def swap_rows(piece):
        idx, start, count = row_pieces[piece]
        which = pl.ds(start, count)
        return remote(part_own.at[idx, which], row_recv.at[idx, which], part_sems.at[2, piece], part_sems.at[3, piece], beside)

    def add_part(lo, count):
        swap_part(lo, count).wait()
        which = pl.ds(lo, count)
        part_own[which] += part_recv[which]

    start_loads(0, 0)
    for idx in range(2):
        load_raw(idx).start()
        swap_raw(idx).start()
    steps = num + 2
    zero_row = jnp.zeros((width, lanes), BF16)
    for slot in range(3):
        g_own[slot, edge_row] = zero_row
    for slot in range(2):
        g_oth[slot, edge_row] = zero_row
        z_own[slot, edge_row] = zero_row
        z_oth[slot, edge_row] = zero_row
    for side in range(3):
        for row in (0, 1, rows + 2, rows + 3):
            shifted[side, row] = zero_row
    tail = pl.ds(grad_rows, 8)
    for idx in range(4):
        part_own[idx, tail] = jnp.zeros((8, lanes), F32)
        part_send[idx, tail] = jnp.zeros((8, lanes), F32)

    @pl.loop(0, steps)
    def _(step):
        @pl.when(step >= 1)
        def _():
            for rel in range(3):
                pl.semaphore_wait(free_sem.at[rel], 1)

        @pl.when(step + 1 < num)
        def _():
            start_loads(0, step + 1)

        @pl.when(step < num)
        def _():
            start_loads(1, step)
            wait_loads(0, step)
            dst = g_own.at[step % 3]

            @pl.loop(0, rows // CONV_ROWS)
            def _(k):
                dst[pl.ds(1 + k * CONV_ROWS, CONV_ROWS)] = dense(0, step % 2, k * CONV_ROWS, CONV_ROWS)

            for copy in g_exchange(step)[:2]:
                copy.start()

        @pl.when(step == 0)
        def _():
            build_weights()
            acc1[...] = jnp.zeros_like(acc1)
            acc2[...] = jnp.zeros_like(acc2)
            db_ref[...] = jnp.zeros_like(db_ref)

        @pl.when((step >= 1) & (step <= num))
        def _():
            img = step - 1
            start_loads(2, img)
            wait_loads(1, img)
            prepare(1, img)
            copies = g_exchange(img)
            halo = arrive(copies)
            copies[1].wait()
            first(img, halo)
            for copy in z_exchange(img)[:2]:
                copy.start()
            for part in kgrad((g_own.at[img % 3], g_oth.at[img % 2]), acc2, 0):
                part()

            @pl.when(img == num - 1)
            def _():
                collect(acc2, 0, 2)
                collect(acc2, 1, 3)
                part_own[2, tail] = db_ref[...]
                part_send[2, tail] = pltpu.roll(db_ref[...], half, 1)
                swap_part(2, 2).start()

        @pl.when(step >= 2)
        def _():
            img = step - 2
            wait_loads(2, img)
            prepare(2, img)

            @pl.when(img >= 1)
            def _():
                finish_out(img - 1)

            @pl.when(img == num - 2)
            def _():
                add_part(2, 2)
                swap_rows(0).start()

            copies = z_exchange(img)
            copies[1].wait()
            for part in kgrad((z_own.at[img % 2],), acc1, 0):
                part()

            @pl.when(img == num - 1)
            def _():
                collect(acc1, 0, 0)
                swap_part(0, 1).start()
                add_part(0, 1)
                swap_rows(2).start()

            halo = arrive(copies)

            @pl.when(img == num - 2)
            def _():
                swap_rows(1).start()

            @pl.when(img == num - 1)
            def _():
                swap_rows(3).start()

            inner, outer = kgrad((z_oth.at[img % 2],), acc1, lanes)
            inner()
            second(img, halo)
            swap_out(img).start()
            outer()

        @pl.when(step + 1 < steps)
        def _():
            for rel, peer in enumerate(peers):
                pl.semaphore_signal(free_sem.at[rel], inc=1, device_id=peer, device_id_type=MESH)

    collect(acc1, 1, 1)
    swap_part(1, 1).start()
    finish_out(num - 1)
    swap_rows(0).wait()
    swap_rows(1).wait()
    dw2_ref[...] = part_own[pl.ds(2, 2)] + row_recv[pl.ds(2, 2)]
    done, late = pl.ds(0, 2 * third), pl.ds(2 * third, third)
    dw1_rest_ref[pl.ds(0, third)] = part_own[0, late]
    swap_part(1, 1).wait()
    inside = pl.ds(0, grad_rows)
    dw1_rest_ref[pl.ds(third, grad_rows)] = part_own[1, inside] + part_recv[1, inside]
    swap_rows(2).wait()
    swap_rows(3).wait()
    dw1_ref[...] = part_own[0, done] + row_recv[0, done]


def unpack(num, packed, grad, out_hbm, grad_out, bias_out, out, bias, store_sem, grad_sem):
    core = lax.axis_index("tp") % 2
    depth, half = out.shape[0], out.shape[-1]

    def stores(i):
        slot = i % depth
        return [pltpu.make_async_copy(out.at[slot, side], out_hbm.at[side, i], store_sem.at[slot, side]) for side in range(2)]

    chip = lax.axis_index("tp") // 2
    inside = pl.ds(0, TAPS * half)
    store_grads = [
        pltpu.make_async_copy(grad.at[side, inside], grad_out.at[:, pl.ds(tile * 2 * half, 2 * half)], grad_sem.at[tile])
        for tile, side in enumerate((chip, 1 - chip))
    ]
    store_bias = pltpu.make_async_copy(bias, bias_out, grad_sem.at[2])
    for copy in store_grads:
        copy.start()
    bias[...] = jnp.sum(grad[0, TAPS * half:, :half], axis=0, keepdims=True)
    store_bias.start()

    @pl.loop(0, num)
    def _(i):
        slot = i % depth

        @pl.when(i >= depth)
        def _():
            for copy in stores(i - depth):
                copy.wait()

        out[slot, core] = packed[i, ..., :half]
        out[slot, 1 - core] = packed[i, ..., half:]
        for copy in stores(i):
            copy.start()

    for i in range(num - depth, num):
        for copy in stores(i):
            copy.wait()
    for copy in store_grads + [store_bias]:
        copy.wait()


def solution(mesh):
    def local_step(x_in, act_saved, w_one, w_two, d_out):
        images, rows, width, half = x_in.shape
        num = images // 2
        lanes = 2 * half
        swap_rows = [(0, 1), (1, 0)]
        third = TAPS * half // 3
        part = pltpu.VMEM((4, TAPS * half + 8, lanes), F32)
        pad = (rows + 2, width, lanes)
        dma = pltpu.SemaphoreType.DMA
        hbm = pl.BlockSpec(memory_space=pltpu.HBM)
        vmem = pl.BlockSpec(memory_space=pltpu.VMEM)
        packed, near, rest, grad_two = pl.pallas_call(
            lambda *refs: body(num, rows, width, *refs),
            out_shape=(
                jax.ShapeDtypeStruct((num, rows, width, lanes), BF16),
                jax.ShapeDtypeStruct((TAPS * half - third, lanes), F32),
                jax.ShapeDtypeStruct((TAPS * half + third, lanes), F32),
                jax.ShapeDtypeStruct((2, TAPS * half + 8, lanes), F32),
            ),
            in_specs=[hbm] * 5,
            out_specs=[vmem] * 4,
            scratch_shapes=[
                pltpu.VMEM((4 * half, TAPS * lanes), F32),
                pltpu.VMEM((4 * half, TAPS * lanes), F32),
                pltpu.VMEM((8, lanes), F32),
                pltpu.VMEM((2,) + w_one.shape, BF16),
                pltpu.VMEM((2,) + w_one.shape, BF16),
                pltpu.VMEM((2, 3 * 4 * half, 3 * lanes), BF16),
                part, part, part, part,
                pltpu.VMEM((3, 2, rows, width, half), BF16),
                pltpu.VMEM((3, 2, rows, width, half), BF16),
                pltpu.VMEM((3,) + pad, BF16),
                pltpu.VMEM((2,) + pad, BF16),
                pltpu.VMEM((2,) + pad, BF16),
                pltpu.VMEM((2,) + pad, BF16),
                pltpu.VMEM((3, rows + 4, width, lanes), BF16),
                pltpu.VMEM((2, rows, width, lanes), BF16),
                pltpu.VMEM((2, rows, width, lanes), BF16),
                dma((3, 2)), dma((3, 2)), dma((3, 2)),
                dma((3, 2)), dma((3, 2)), dma((3, 2)), dma((3, 2)),
                dma((2,)), dma((2,)),
                dma((2,)), dma((2,)), dma((2,)), dma((4, 4)),
                pltpu.SemaphoreType.REGULAR((3,)),
            ],
            compiler_params=pltpu.CompilerParams(collective_id=0, has_side_effects=True, vmem_limit_bytes=32 * 1024 * 1024),
        )(x_in, act_saved, d_out, *(pltpu.with_memory_space_constraint(w, pltpu.HBM) for w in (w_one, w_two)))

        depth = 8
        d_x, grad_two, bias = pl.pallas_call(
            lambda *refs: unpack(num, *refs),
            out_shape=(
                jax.ShapeDtypeStruct((2, num, rows, width, half), BF16),
                jax.ShapeDtypeStruct((TAPS * half, 4 * half), F32),
                jax.ShapeDtypeStruct((1, half), F32),
            ),
            in_specs=[vmem] * 2,
            out_specs=[hbm] * 3,
            scratch_shapes=[
                pltpu.VMEM((depth, 2, rows, width, half), BF16),
                pltpu.VMEM((1, half), F32),
                dma((depth, 2)), dma((3,)),
            ],
            compiler_params=pltpu.CompilerParams(vmem_limit_bytes=14 * 1024 * 1024),
            cost_estimate=pl.CostEstimate(flops=10**10, bytes_accessed=5 * 10**7, transcendentals=0),
        )(packed, grad_two)
        rest = rest + lax.ppermute(rest, "sp", swap_rows)
        near, far = jnp.concatenate([near, rest[:third]], axis=0), rest[third:]
        on_left = lax.axis_index("tp") < 2
        grad_one = jnp.concatenate([jnp.where(on_left, near, far), jnp.where(on_left, far, near)], axis=1)
        return d_x.reshape(x_in.shape), grad_one.reshape(w_one.shape), grad_two.reshape(w_two.shape), bias.reshape(half)

    act_spec = P("dp", "sp", None, "tp")
    kern_spec = P(None, None, "tp", None)
    grad_spec = P("dp", None, "tp", None)
    return jax.shard_map(local_step, mesh=mesh, in_specs=(act_spec, act_spec, kern_spec, kern_spec, act_spec), out_specs=(act_spec, grad_spec, grad_spec, P(("dp", "tp"))), check_vma=False)
```

```python
import jax
import jax.numpy as jnp
from jax import lax
from jax.experimental import pallas as pl
from jax.experimental.pallas import tpu as pltpu
from jax.sharding import PartitionSpec as P

MESH = pl.DeviceIdType.MESH
F32, BF16 = jnp.float32, jnp.bfloat16
TAPS = 9
CONV_ROWS = 16
GRAD_ROWS = 32


def body(num, rows, width, x_hbm, a_hbm, y_hbm, w1_hbm, w2_hbm, packed, dw1_ref, dw1_rest_ref, dw2_ref,
         acc1, acc2, db_ref, raw_own, raw_rem, weights, part_own, part_send, part_recv, row_recv, nat_own, nat_rem, g_own, g_oth, z_own, z_oth, shifted, out_own, out_rem,
         load_sem, push_send, push_recv, g_send, g_recv, z_send, z_recv, out_send, out_recv, raw_sem, raw_send, raw_recv, part_sems, free_sem):
    dp, sp, tp = lax.axis_index("dp"), lax.axis_index("sp"), lax.axis_index("tp")
    core, chip = tp % 2, tp // 2
    partner = (dp, sp, tp + 1 - 2 * core)
    across = (dp, sp, (tp + 2) % 4)
    beside = (dp, 1 - sp, tp)
    peers = (partner, across, beside)
    half = 64
    lanes = 2 * half
    edge_row = (rows + 1) * sp
    halo_row = (rows + 1) * (1 - sp)
    halo_src = rows - (rows - 1) * sp
    m_conv = CONV_ROWS * width
    m_grad = GRAD_ROWS * width

    barrier = pltpu.get_barrier_semaphore()
    for peer in peers:
        pl.semaphore_signal(barrier, inc=1, device_id=peer, device_id_type=MESH)
    pl.semaphore_wait(barrier, 3)

    def remote(src, dst, send, recv, peer):
        return pltpu.make_async_remote_copy(src_ref=src, dst_ref=dst, send_sem=send, recv_sem=recv, device_id=peer, device_id_type=MESH)

    sources = (y_hbm, a_hbm, x_hbm)

    def loads(kind, img):
        slot = img % 2
        local = pltpu.make_async_copy(sources[kind].at[core * num + img], nat_own.at[kind, slot], load_sem.at[kind, slot])
        push = remote(sources[kind].at[(1 - core) * num + img], nat_rem.at[kind, slot], push_send.at[kind, slot], push_recv.at[kind, slot], partner)
        return local, push

    def start_loads(kind, img):
        for copy in loads(kind, img):
            copy.start()

    def wait_loads(kind, img):
        for copy in loads(kind, img):
            copy.wait()

    def exchange(own, own_slot, oth, oth_slot, send, recv, sem_slot):
        return (
            remote(own.at[own_slot, pl.ds(1, rows)], oth.at[oth_slot, pl.ds(1, rows)], send.at[0, sem_slot], recv.at[0, sem_slot], across),
            remote(own.at[own_slot, halo_src], own.at[own_slot, edge_row], send.at[1, sem_slot], recv.at[1, sem_slot], beside),
            remote(oth.at[oth_slot, halo_src], oth.at[oth_slot, edge_row], send.at[2, sem_slot], recv.at[2, sem_slot], beside),
        )

    def g_exchange(img):
        return exchange(g_own, img % 3, g_oth, img % 2, g_send, g_recv, img % 2)

    def z_exchange(img):
        return exchange(z_own, img % 2, z_oth, img % 2, z_send, z_recv, img % 2)

    def swap_out(img):
        slot = img % 2
        return remote(out_own.at[slot], out_rem.at[slot], out_send.at[slot], out_recv.at[slot], partner)

    def finish_out(img):
        slot = img % 2
        swap_out(img).wait()

        @pl.loop(0, rows // CONV_ROWS)
        def _(k):
            block = pl.ds(k * CONV_ROWS, CONV_ROWS)
            lane = lax.broadcasted_iota(jnp.int32, (CONV_ROWS, width, lanes), 2)
            packed[img, block] = jnp.where(lane < half, out_own[slot, block], out_rem[slot, block])

    def dense(kind, slot, r0, count):
        mine = nat_own[kind, slot, pl.ds(r0, count)]
        theirs = nat_rem[kind, slot, pl.ds(r0, count)]
        return jnp.concatenate([mine, theirs], axis=-1)

    col = lax.broadcasted_iota(jnp.int32, (m_conv, lanes), 0) % width
    at_first = col == 0
    at_last = col == width - 1

    def from_right(v):
        return jnp.where(at_last, 0.0, pltpu.roll(v, m_conv - 1, 0))

    def from_left(v):
        return jnp.where(at_first, 0.0, pltpu.roll(v, 1, 0))

    def prepare(kind, img):
        @pl.loop(0, rows // CONV_ROWS)
        def _(k):
            r0 = k * CONV_ROWS
            v = dense(kind, img % 2, r0, CONV_ROWS)
            flat = v.reshape(m_conv, lanes).astype(F32)
            shifted[1, pl.ds(r0 + 2, CONV_ROWS)] = v
            shifted[0, pl.ds(r0 + 2, CONV_ROWS)] = from_left(flat).astype(BF16).reshape(v.shape)
            shifted[2, pl.ds(r0 + 2, CONV_ROWS)] = from_right(flat).astype(BF16).reshape(v.shape)

    def both(own, oth, r, count):
        shape = (count * width, lanes)
        return [own[pl.ds(r, count)].reshape(shape), oth[pl.ds(r, count)].reshape(shape)]

    def conv(own, oth, r0, w_ref):
        lhs = jnp.concatenate(sum((both(own, oth, r0 + 2 - kh, CONV_ROWS) for kh in range(3)), []), axis=-1)
        out = jnp.dot(lhs, w_ref[...], preferred_element_type=F32)
        return out[:, lanes:2 * lanes] + from_right(out[:, :lanes]) + from_left(out[:, 2 * lanes:])

    def kgrad(sources, acc, first_row):
        dst = pl.ds(first_row, lanes * len(sources))

        def piece(r, count):
            shape = (count * width, lanes)
            lhs = jnp.concatenate([src[pl.ds(r, count)].reshape(shape) for src in sources], axis=-1)
            taps = [shifted[kw, pl.ds(r + kh, count)].reshape(shape) for kh in range(3) for kw in range(3)]
            rhs = jnp.concatenate(taps, axis=-1)
            acc[dst] += lax.dot_general(lhs, rhs, (((0,), (0,)), ((), ())), preferred_element_type=F32)

        def inner():
            @pl.loop(0, rows // GRAD_ROWS)
            def _(k):
                piece(1 + k * GRAD_ROWS, GRAD_ROWS)

        return inner, lambda: piece(halo_row, 1)

    last_block = rows // CONV_ROWS - 1

    def blocks(halo, step):
        @pl.loop(0, last_block + 1)
        def _(k):
            @pl.when(k == last_block)
            def _():
                halo.wait()

            step((k + (last_block - 2 * k) * sp) * CONV_ROWS)

    def first(img, halo):
        own, oth = g_own.at[img % 3], g_oth.at[img % 2]
        out = z_own.at[img % 2]

        def step(r0):
            d_act = conv(own, oth, r0, weights.at[1])
            live = shifted[1, pl.ds(r0 + 2, CONV_ROWS)].reshape(m_conv, lanes).astype(F32) > 0
            masked = jnp.where(live, d_act, 0.0)
            db_ref[...] += jnp.sum(masked.reshape(m_conv // 8, 8, lanes), axis=0)
            out[pl.ds(1 + r0, CONV_ROWS)] = masked.astype(BF16).reshape(CONV_ROWS, width, lanes)

        blocks(halo, step)

    def second(img, halo):
        own, oth = z_own.at[img % 2], z_oth.at[img % 2]
        skip = g_own.at[img % 3]
        slot = img % 2

        def step(r0):
            d_x = conv(own, oth, r0, weights.at[0])
            d_x = d_x + skip[pl.ds(1 + r0, CONV_ROWS)].reshape(m_conv, lanes).astype(F32)
            out_own[slot, pl.ds(r0, CONV_ROWS)] = d_x.astype(BF16).reshape(CONV_ROWS, width, lanes)

        blocks(halo, step)

    def arrive(copies):
        main, _, forward = copies
        main.wait()
        forward.start()
        return forward

    raw = (w1_hbm, w2_hbm)

    def swap_raw(idx):
        return remote(raw[idx], raw_rem.at[idx], raw_send.at[idx], raw_recv.at[idx], partner)

    def load_raw(idx):
        return pltpu.make_async_copy(raw[idx], raw_own.at[idx], raw_sem.at[idx])

    def local_block(block):
        on_chip = chip if block < 2 else 1 - chip
        on_core = core if block % 2 == 0 else 1 - core
        return pl.multiple_of((2 * on_chip + on_core) * half, half)

    def build_weights():
        for idx in range(2):
            load_raw(idx).wait()
            swap_raw(idx).wait()

            @pl.loop(0, 3)
            def _(kh):
                for kw in range(3):
                    taps = jnp.concatenate([raw_own[idx, kh, kw], raw_rem[idx, kh, kw]], axis=0).T
                    for block in range(4):
                        dst = pl.ds(pl.multiple_of(kh * 4 * half, half) + local_block(block), half)
                        weights[idx, dst, kw * lanes:(kw + 1) * lanes] = taps[block * half:(block + 1) * half]

    grad_rows = TAPS * half

    def collect(acc, side, idx):
        @pl.loop(0, TAPS)
        def _(tap):
            cols = pl.ds(pl.multiple_of(tap * lanes, lanes), lanes)
            firsts = (core, 1 - core)
            pieces = [acc[pl.ds(pl.multiple_of(side * lanes + first * half, half), half), cols] for first in firsts]
            flipped = jnp.concatenate(pieces, axis=0).T
            dst = pl.ds(pl.multiple_of(tap * half, half), half)
            part_own[idx, dst] = flipped[:half]
            part_send[idx, dst] = flipped[half:]

    def swap_part(lo, count):
        which = pl.ds(lo, count)
        return remote(part_send.at[which], part_recv.at[which], part_sems.at[0, lo], part_sems.at[1, lo], partner)

    third = grad_rows // 3
    whole = grad_rows + 8
    row_pieces = ((2, 0, whole), (3, 0, whole), (0, 0, third), (0, third, third))

    def swap_rows(piece):
        idx, start, count = row_pieces[piece]
        which = pl.ds(start, count)
        return remote(part_own.at[idx, which], row_recv.at[idx, which], part_sems.at[2, piece], part_sems.at[3, piece], beside)

    def add_part(lo, count):
        swap_part(lo, count).wait()
        which = pl.ds(lo, count)
        part_own[which] += part_recv[which]

    start_loads(0, 0)
    for idx in range(2):
        load_raw(idx).start()
        swap_raw(idx).start()
    steps = num + 2
    zero_row = jnp.zeros((width, lanes), BF16)
    for slot in range(3):
        g_own[slot, edge_row] = zero_row
    for slot in range(2):
        g_oth[slot, edge_row] = zero_row
        z_own[slot, edge_row] = zero_row
        z_oth[slot, edge_row] = zero_row
    for side in range(3):
        for row in (0, 1, rows + 2, rows + 3):
            shifted[side, row] = zero_row
    tail = pl.ds(grad_rows, 8)
    for idx in range(4):
        part_own[idx, tail] = jnp.zeros((8, lanes), F32)
        part_send[idx, tail] = jnp.zeros((8, lanes), F32)

    @pl.loop(0, steps)
    def _(step):
        @pl.when(step >= 1)
        def _():
            for rel in range(3):
                pl.semaphore_wait(free_sem.at[rel], 1)

        @pl.when(step + 1 < num)
        def _():
            start_loads(0, step + 1)

        @pl.when(step < num)
        def _():
            start_loads(1, step)
            wait_loads(0, step)
            dst = g_own.at[step % 3]

            @pl.loop(0, rows // CONV_ROWS)
            def _(k):
                dst[pl.ds(1 + k * CONV_ROWS, CONV_ROWS)] = dense(0, step % 2, k * CONV_ROWS, CONV_ROWS)

            for copy in g_exchange(step)[:2]:
                copy.start()

        @pl.when(step == 0)
        def _():
            build_weights()
            acc1[...] = jnp.zeros_like(acc1)
            acc2[...] = jnp.zeros_like(acc2)
            db_ref[...] = jnp.zeros_like(db_ref)

        @pl.when((step >= 1) & (step <= num))
        def _():
            img = step - 1
            start_loads(2, img)
            wait_loads(1, img)
            prepare(1, img)
            copies = g_exchange(img)
            halo = arrive(copies)
            copies[1].wait()
            first(img, halo)
            for copy in z_exchange(img)[:2]:
                copy.start()
            for part in kgrad((g_own.at[img % 3], g_oth.at[img % 2]), acc2, 0):
                part()

            @pl.when(img == num - 1)
            def _():
                collect(acc2, 0, 2)
                collect(acc2, 1, 3)
                part_own[2, tail] = db_ref[...]
                part_send[2, tail] = pltpu.roll(db_ref[...], half, 1)
                swap_part(2, 2).start()

        @pl.when(step >= 2)
        def _():
            img = step - 2
            wait_loads(2, img)
            prepare(2, img)

            @pl.when(img >= 1)
            def _():
                finish_out(img - 1)

            @pl.when(img == num - 2)
            def _():
                add_part(2, 2)
                swap_rows(0).start()

            copies = z_exchange(img)
            copies[1].wait()
            for part in kgrad((z_own.at[img % 2],), acc1, 0):
                part()

            @pl.when(img == num - 1)
            def _():
                collect(acc1, 0, 0)
                swap_part(0, 1).start()
                add_part(0, 1)
                swap_rows(2).start()

            halo = arrive(copies)

            @pl.when(img == num - 2)
            def _():
                swap_rows(1).start()

            @pl.when(img == num - 1)
            def _():
                swap_rows(3).start()

            inner, outer = kgrad((z_oth.at[img % 2],), acc1, lanes)
            inner()
            second(img, halo)
            swap_out(img).start()
            outer()

        @pl.when(step + 1 < steps)
        def _():
            for rel, peer in enumerate(peers):
                pl.semaphore_signal(free_sem.at[rel], inc=1, device_id=peer, device_id_type=MESH)

    collect(acc1, 1, 1)
    swap_part(1, 1).start()
    finish_out(num - 1)
    swap_rows(0).wait()
    swap_rows(1).wait()
    dw2_ref[...] = part_own[pl.ds(2, 2)] + row_recv[pl.ds(2, 2)]
    done, late = pl.ds(0, 2 * third), pl.ds(2 * third, third)
    dw1_rest_ref[pl.ds(0, third)] = part_own[0, late]
    swap_part(1, 1).wait()
    inside = pl.ds(0, grad_rows)
    dw1_rest_ref[pl.ds(third, grad_rows)] = part_own[1, inside] + part_recv[1, inside]
    swap_rows(2).wait()
    swap_rows(3).wait()
    dw1_ref[...] = part_own[0, done] + row_recv[0, done]


def unpack(num, packed, grad, out_hbm, grad_out, bias_out, out, bias, store_sem, grad_sem):
    core = lax.axis_index("tp") % 2
    depth, half = out.shape[0], out.shape[-1]

    def stores(i):
        slot = i % depth
        return [pltpu.make_async_copy(out.at[slot, side], out_hbm.at[side, i], store_sem.at[slot, side]) for side in range(2)]

    chip = lax.axis_index("tp") // 2
    inside = pl.ds(0, TAPS * half)
    store_grads = [
        pltpu.make_async_copy(grad.at[side, inside], grad_out.at[:, pl.ds(tile * 2 * half, 2 * half)], grad_sem.at[tile])
        for tile, side in enumerate((chip, 1 - chip))
    ]
    store_bias = pltpu.make_async_copy(bias, bias_out, grad_sem.at[2])
    for copy in store_grads:
        copy.start()
    bias[...] = jnp.sum(grad[0, TAPS * half:, :half], axis=0, keepdims=True)
    store_bias.start()

    @pl.loop(0, num)
    def _(i):
        slot = i % depth

        @pl.when(i >= depth)
        def _():
            for copy in stores(i - depth):
                copy.wait()

        out[slot, core] = packed[i, ..., :half]
        out[slot, 1 - core] = packed[i, ..., half:]
        for copy in stores(i):
            copy.start()

    for i in range(num - depth, num):
        for copy in stores(i):
            copy.wait()
    for copy in store_grads + [store_bias]:
        copy.wait()


def solution(mesh):
    def local_step(x_in, act_saved, w_one, w_two, d_out):
        images, rows, width, half = x_in.shape
        num = images // 2
        lanes = 2 * half
        swap_rows = [(0, 1), (1, 0)]
        third = TAPS * half // 3
        part = pltpu.VMEM((4, TAPS * half + 8, lanes), F32)
        pad = (rows + 2, width, lanes)
        dma = pltpu.SemaphoreType.DMA
        hbm = pl.BlockSpec(memory_space=pltpu.HBM)
        vmem = pl.BlockSpec(memory_space=pltpu.VMEM)
        packed, near, rest, grad_two = pl.pallas_call(
            lambda *refs: body(num, rows, width, *refs),
            out_shape=(
                jax.ShapeDtypeStruct((num, rows, width, lanes), BF16),
                jax.ShapeDtypeStruct((TAPS * half - third, lanes), F32),
                jax.ShapeDtypeStruct((TAPS * half + third, lanes), F32),
                jax.ShapeDtypeStruct((2, TAPS * half + 8, lanes), F32),
            ),
            in_specs=[hbm] * 5,
            out_specs=[vmem] * 4,
            scratch_shapes=[
                pltpu.VMEM((4 * half, TAPS * lanes), F32),
                pltpu.VMEM((4 * half, TAPS * lanes), F32),
                pltpu.VMEM((8, lanes), F32),
                pltpu.VMEM((2,) + w_one.shape, BF16),
                pltpu.VMEM((2,) + w_one.shape, BF16),
                pltpu.VMEM((2, 3 * 4 * half, 3 * lanes), BF16),
                part, part, part, part,
                pltpu.VMEM((3, 2, rows, width, half), BF16),
                pltpu.VMEM((3, 2, rows, width, half), BF16),
                pltpu.VMEM((3,) + pad, BF16),
                pltpu.VMEM((2,) + pad, BF16),
                pltpu.VMEM((2,) + pad, BF16),
                pltpu.VMEM((2,) + pad, BF16),
                pltpu.VMEM((3, rows + 4, width, lanes), BF16),
                pltpu.VMEM((2, rows, width, lanes), BF16),
                pltpu.VMEM((2, rows, width, lanes), BF16),
                dma((3, 2)), dma((3, 2)), dma((3, 2)),
                dma((3, 2)), dma((3, 2)), dma((3, 2)), dma((3, 2)),
                dma((2,)), dma((2,)),
                dma((2,)), dma((2,)), dma((2,)), dma((4, 4)),
                pltpu.SemaphoreType.REGULAR((3,)),
            ],
            compiler_params=pltpu.CompilerParams(collective_id=0, has_side_effects=True, vmem_limit_bytes=32 * 1024 * 1024),
        )(x_in, act_saved, d_out, *(pltpu.with_memory_space_constraint(w, pltpu.HBM) for w in (w_one, w_two)))

        depth = 12
        d_x, grad_two, bias = pl.pallas_call(
            lambda *refs: unpack(num, *refs),
            out_shape=(
                jax.ShapeDtypeStruct((2, num, rows, width, half), BF16),
                jax.ShapeDtypeStruct((TAPS * half, 4 * half), F32),
                jax.ShapeDtypeStruct((1, half), F32),
            ),
            in_specs=[vmem] * 2,
            out_specs=[hbm] * 3,
            scratch_shapes=[
                pltpu.VMEM((depth, 2, rows, width, half), BF16),
                pltpu.VMEM((1, half), F32),
                dma((depth, 2)), dma((3,)),
            ],
            compiler_params=pltpu.CompilerParams(vmem_limit_bytes=14 * 1024 * 1024),
            cost_estimate=pl.CostEstimate(flops=10**10, bytes_accessed=5 * 10**7, transcendentals=0),
        )(packed, grad_two)
        rest = rest + lax.ppermute(rest, "sp", swap_rows)
        near, far = jnp.concatenate([near, rest[:third]], axis=0), rest[third:]
        on_left = lax.axis_index("tp") < 2
        grad_one = jnp.concatenate([jnp.where(on_left, near, far), jnp.where(on_left, far, near)], axis=1)
        return d_x.reshape(x_in.shape), grad_one.reshape(w_one.shape), grad_two.reshape(w_two.shape), bias.reshape(half)

    act_spec = P("dp", "sp", None, "tp")
    kern_spec = P(None, None, "tp", None)
    grad_spec = P("dp", None, "tp", None)
    return jax.shard_map(local_step, mesh=mesh, in_specs=(act_spec, act_spec, kern_spec, kern_spec, act_spec), out_specs=(act_spec, grad_spec, grad_spec, P(("dp", "tp"))), check_vma=False)
```
